256 devices in a mesh: dp: 64 (over z, y, core), mp: 4 (over x).
Axes of the slice: x: 4, y: 4, z: 8, core: 2. Of those that a mesh axis runs over, the one named last changes fastest.
Arguments:
- patches: bfloat16 [131072, 1024], P('dp'), may hold values from -110 to 110
- dest_owner: int32 [8192], P('dp'), may hold values from 0 to 63, as said below
- dest_slot: int32 [8192], P('dp'), may hold values from 0 to 127
- packed_image: int32 [8192], P('dp'), may hold values from -1 to 15, as said below
- w_query: bfloat16 [1024, 1024], P(None, 'mp'), may hold values from -0.328125 to 0.328125
- w_key: bfloat16 [1024, 1024], P(None, 'mp'), may hold values from -1.9375 to 1.9375
- w_value: bfloat16 [1024, 1024], P(None, 'mp'), may hold values from -0.1875 to 0.1875
- w_out: bfloat16 [1024, 1024], P('mp'), may hold values from -0.1875 to 0.1875
Outputs:
- packed_out: bfloat16 [131072, 1024], P('dp', 'mp')
- pooled_out: bfloat16 [1024, 1024], P('dp', 'mp')
The draws below stay inside these ranges and needn't reach their ends.
Inputs may be any that keep to these rules, and one draw needn't show every extreme that they name: dest_owner and dest_slot take the tiles of all indices of dp one to one onto the 128 tile slots of every packed sequence; each index of dp holds exactly 2 tiles for each packed sequence. `packed_image`: in every packed sequence the images 0, 1, 2 and so on lie on consecutive tile slots from slot 0 in the order of their numbers, each on 8 to 16 slots; fewer than 16 slots stay empty after the last image and hold -1.
All inputs are finite; a program needn't handle non-finite values.
Results may differ from the reference program's by a relative error of at most 0.0075.
Values may be sent and summed in bfloat16 or wider, within the bound.
No kernel may reach another device: no remote copies, remote signals or barrier semaphores. Data moves between devices by JAX's collectives and lax.ppermute only.
A program may use at most 128 MiB of HBM per device.

```python
import math
import jax
import jax.numpy as jnp
from jax import lax

D = 1024
HEADS = 16
HEAD_DIM = 64
TILE = 16
MAXT = 16
MINT = 8
SLOTS = 128
IMG_OWN = 16
ROWS = 131072
N_DP = 64
N_MP = 4


def layout(key):
    per_pair = SLOTS // N_DP
    owner_keys = jax.random.split(jax.random.fold_in(key, 101), N_DP)
    source_keys = jax.random.split(jax.random.fold_in(key, 102), N_DP)
    slot_perm = jax.vmap(lambda single: jax.random.permutation(single, SLOTS))(owner_keys).astype(jnp.int32)
    tile_perm = jax.vmap(lambda single: jax.random.permutation(single, SLOTS))(source_keys).astype(jnp.int32)
    sources = jnp.arange(N_DP, dtype=jnp.int32)[:, None]
    owners = tile_perm // per_pair
    within = tile_perm % per_pair
    column = (sources - owners) % N_DP + N_DP * within
    slots = slot_perm[owners, column]
    owner_ids = jnp.arange(N_DP, dtype=jnp.int32)
    image_tiles = jax.random.randint(jax.random.fold_in(key, 104), (N_DP, IMG_OWN), MINT, MAXT + 1)
    biggest = jax.random.randint(jax.random.fold_in(key, 105), (), 0, N_DP)
    fullest = (biggest + 1) % N_DP
    image_tiles = jnp.where((owner_ids == fullest)[:, None], MINT, image_tiles)
    image_tiles = image_tiles.at[:, 0].set(jnp.where(owner_ids == biggest, MAXT, image_tiles[:, 0]))
    kept = jnp.cumsum(image_tiles, axis=1) <= SLOTS
    image_tiles = jnp.where(kept, image_tiles, 0)
    ends = jnp.cumsum(image_tiles, axis=1)
    tile_ids = jnp.arange(SLOTS, dtype=jnp.int32)
    finished = jnp.sum((tile_ids[None, :, None] >= ends[:, None, :]).astype(jnp.int32), axis=2)
    image = jnp.where(tile_ids[None, :] < ends[:, -1:], finished, -1)
    return (owners.reshape(-1).astype(jnp.int32), slots.reshape(-1).astype(jnp.int32), image.reshape(-1).astype(jnp.int32))


def draw_dest_owner(key, part):
    return layout(key)[0]


def draw_dest_slot(key, part):
    return layout(key)[1]


def draw_packed_image(key, part):
    return layout(key)[2]


def draw_patches(key, part):
    owners = layout(key)[0]
    row_owner = jnp.repeat(owners, TILE)
    base = jax.random.truncated_normal(jax.random.fold_in(key, 111), -4.0, 4.0, (D,))
    region = jax.random.truncated_normal(jax.random.fold_in(key, 112), -4.0, 4.0, (N_DP, D))
    noise = jax.random.truncated_normal(jax.random.fold_in(key, 113), -4.0, 4.0, (ROWS, D))
    rows = base[None, :] + 0.7 * region[row_owner] + noise
    return rows.astype(jnp.bfloat16)


def query_key(key):
    first_draw = jax.random.truncated_normal(jax.random.fold_in(key, 201), -4.0, 4.0, (D, D)) / math.sqrt(D)
    second_draw = jax.random.truncated_normal(jax.random.fold_in(key, 202), -4.0, 4.0, (D, D)) / math.sqrt(D)
    return (first_draw, second_draw)


def draw_w_query(key, part):
    first_draw, second_draw = query_key(key)
    return first_draw.astype(jnp.bfloat16)


def draw_w_key(key, part):
    first_draw, second_draw = query_key(key)
    return second_draw.astype(jnp.bfloat16)


def level_of(rng, extent, pieces, low, high):
    level, own = 1.0, jax.random.fold_in(rng, 6)
    for dim, parts in pieces:
        steps = jnp.exp(jax.random.uniform(jax.random.fold_in(own, dim), (parts,), jnp.float32, low / len(pieces), high / len(pieces)))
        level = level * jnp.repeat(steps, extent[dim] // parts).reshape([-1 if axis == dim else 1 for axis in range(len(extent))])
    return level


def bell_draw(stream_key, dims, deviation, most, cuts=(), kind=jnp.bfloat16):
    entries = deviation * jax.random.normal(stream_key, dims, jnp.float32)
    if cuts:
        entries = entries * level_of(stream_key, dims, cuts, -0.22, 0.18)
    return jnp.clip(entries, -most, most).astype(kind)


def setup_inputs(seed: int = 0) -> dict:
    streams_of = jax.random.split(jax.random.key(seed), 9)
    return {
        "patches": draw_patches(jax.random.fold_in(streams_of[8], 71), 0),
        "dest_owner": draw_dest_owner(jax.random.fold_in(streams_of[8], 71), 0),
        "dest_slot": draw_dest_slot(jax.random.fold_in(streams_of[8], 71), 0),
        "packed_image": draw_packed_image(jax.random.fold_in(streams_of[8], 71), 0),
        "w_query": draw_w_query(jax.random.fold_in(streams_of[8], 71), 0),
        "w_key": draw_w_key(jax.random.fold_in(streams_of[8], 71), 0),
        "w_value": bell_draw(streams_of[6], (D, D), D ** -0.5, 0.1875, ((1, 4),)),
        "w_out": bell_draw(streams_of[7], (D, D), D ** -0.5, 0.1875, ((0, 4),)),
    }


EPSILON = 1e-06

def normalize(rows):
    values = rows.astype(jnp.float32)
    centred = values - lax.optimization_barrier(jnp.mean(values, axis=-1, keepdims=True))
    spread = lax.optimization_barrier(jnp.mean(centred * centred, axis=-1, keepdims=True))
    return (centred * lax.rsqrt(spread + EPSILON)).astype(jnp.bfloat16)

def attend(queries, key_rows, values, allowed, present):
    scores = jnp.einsum('qhd,khd->hqk', queries.astype(jnp.float32), key_rows.astype(jnp.float32)) * HEAD_DIM ** (-0.5)
    masked = jnp.where(allowed[None], scores, -1e+30)
    peak = lax.optimization_barrier(jnp.max(masked, axis=-1, keepdims=True))
    raised = jnp.where(allowed[None], jnp.exp(scores - peak), 0.0)
    denominator = lax.optimization_barrier(jnp.sum(raised, axis=-1, keepdims=True))
    denominator = jnp.where(present[None, :, None], denominator, 1.0)
    weights = (raised / denominator).astype(jnp.bfloat16)
    return jnp.einsum('hqk,khd->qhd', weights.astype(jnp.float32), values.astype(jnp.float32)).astype(jnp.bfloat16)

def reference(patches, dest_owner, dest_slot, packed_image, w_query, w_key, w_value, w_out):
    seq_rows = SLOTS * TILE
    target = dest_owner * SLOTS + dest_slot
    source_of = jnp.argsort(target).astype(jnp.int32)
    packed = jnp.take(patches.reshape(N_DP * SLOTS, TILE, D), source_of, axis=0).reshape(N_DP, seq_rows, D)
    segment_ids = packed_image.reshape(N_DP, SLOTS)
    labels = jnp.arange(IMG_OWN, dtype=jnp.int32)

    def owner_block(inputs):
        rows, seg_tiles = inputs
        segment = jnp.repeat(seg_tiles, TILE)
        present = segment >= 0
        normed = normalize(rows)
        queries = jnp.dot(normed, w_query, preferred_element_type=jnp.float32).astype(jnp.bfloat16)
        key_rows = jnp.dot(normed, w_key, preferred_element_type=jnp.float32).astype(jnp.bfloat16)
        values = jnp.dot(normed, w_value, preferred_element_type=jnp.float32).astype(jnp.bfloat16)
        queries = queries.reshape(seq_rows, HEADS, HEAD_DIM)
        key_rows = key_rows.reshape(seq_rows, HEADS, HEAD_DIM)
        values = values.reshape(seq_rows, HEADS, HEAD_DIM)
        allowed = (segment[:, None] == segment[None, :]) & present[:, None]
        attended = attend(queries, key_rows, values, allowed, present).reshape(seq_rows, D)
        groups = attended.reshape(seq_rows, N_MP, D // N_MP).astype(jnp.float32)
        out_groups = w_out.reshape(N_MP, D // N_MP, D).astype(jnp.float32)
        head_term = jnp.einsum('rgc,gcd->grd', groups, out_groups)
        rounded = lax.optimization_barrier(head_term.astype(jnp.bfloat16)).astype(jnp.float32)
        projected = lax.optimization_barrier(jnp.sum(rounded, axis=0))
        result_rows = jnp.where(present[:, None], rows.astype(jnp.float32) + projected, 0.0)
        member = (segment[None, :] == labels[:, None]).astype(jnp.float32)
        sums = jnp.dot(member, result_rows, precision=lax.Precision.HIGHEST)
        image_rows = lax.optimization_barrier(jnp.sum(member, axis=1))
        filled = image_rows > 0
        pooled = sums / jnp.maximum(image_rows, 1.0)[:, None]
        local_sum = lax.optimization_barrier(jnp.sum(jnp.where(filled[:, None], pooled, 0.0), axis=0))
        local_count = jnp.sum(filled.astype(jnp.float32))
        return (result_rows.astype(jnp.bfloat16), pooled, filled, local_sum, local_count)
    out_rows, pooled, filled, local_sum, local_count = lax.map(owner_block, (packed, segment_ids))
    centre = lax.optimization_barrier(jnp.sum(local_sum, axis=0)) / jnp.sum(local_count)
    pooled_out = jnp.where(filled[:, :, None], pooled - centre[None, None, :], 0.0).astype(jnp.bfloat16)
    return (out_rows.reshape(N_DP * seq_rows, D), pooled_out.reshape(N_DP * IMG_OWN, D))
```

```python
import functools
import jax
import jax.numpy as jnp
from jax import lax
from jax.experimental import pallas as pl
from jax.experimental.pallas import tpu as pltpu
from jax.sharding import PartitionSpec as P

EPSILON = 1e-06
SLOTS = 128
TILE = 16
D = 1024
PARTS = 4
PW = D // PARTS
PART_SLOTS = SLOTS // PARTS
WIN = PART_SLOTS + 16
ROWS_W = WIN * TILE
IMG = 16
EXTRA = 3 * IMG
HD = 64
MAX_LOCAL = 4
PAY = 72
IMG_ROWS = 256
VMEM = pltpu.CompilerParams(vmem_limit_bytes=56 * 1024 * 1024)


def send_kernel(owner_ref, slot_ref, mp_ref, patch_ref, out_ref, count_ref, place_ref):
    owners = out_ref.shape[0]

    def clear(o, carry):
        count_ref[o] = 0
        return carry

    lax.fori_loop(0, owners, clear, 0)

    def move(t, carry):
        o = owner_ref[t]
        r = count_ref[o]
        count_ref[o] = r + 1
        place_ref[2 * o + r] = slot_ref[t]
        rows = patch_ref[pl.ds(pl.multiple_of(t * TILE, TILE), TILE), :]
        base = pl.multiple_of(r * 2 * TILE, TILE)
        out_ref[o, pl.ds(base, TILE), :] = rows[:, :128]
        out_ref[o, pl.ds(base + TILE, TILE), :] = rows[:, 128:]
        return carry

    lax.fori_loop(0, SLOTS, move, 0)
    row = lax.broadcasted_iota(jnp.int32, (PAY - 64, 128), 0)

    def label(o, carry):
        value = jnp.where(row == 0, place_ref[2 * o], place_ref[2 * o + 1])
        out_ref[o, 64:, :] = value.astype(jnp.float32).astype(jnp.bfloat16)
        return carry

    lax.fori_loop(0, owners, label, 0)


def send_pack(owner, slot, mp, patches, senders):
    return pl.pallas_call(
        send_kernel,
        grid_spec=pltpu.PrefetchScalarGridSpec(
            num_scalar_prefetch=3,
            grid=(1,),
            in_specs=[pl.BlockSpec((SLOTS * TILE, PW), lambda i, a, b, m: (0, m[0]))],
            out_specs=pl.BlockSpec((senders, PAY, 128), lambda i, a, b, m: (0, 0, 0)),
            scratch_shapes=[pltpu.SMEM((senders,), jnp.int32), pltpu.SMEM((2 * senders,), jnp.int32)],
        ),
        out_shape=jax.ShapeDtypeStruct((senders, PAY, 128), jnp.bfloat16),
        compiler_params=VMEM,
        name="send_pack",
    )(owner, slot, mp, patches)


def arrive_kernel(slot_ref, in_ref, out_ref):
    out_ref[PARTS - 1, PART_SLOTS * TILE :, :] = jnp.zeros((ROWS_W - PART_SLOTS * TILE, PW), jnp.bfloat16)

    def move(n, carry):
        t = slot_ref[n]
        s = n // 2
        base = pl.multiple_of((n % 2) * 2 * TILE, TILE)
        left = in_ref[s, pl.ds(base, TILE), :]
        right = in_ref[s, pl.ds(base + TILE, TILE), :]
        part = t // PART_SLOTS
        local = t % PART_SLOTS
        at = pl.multiple_of(local * TILE, TILE)
        out_ref[part, pl.ds(at, TILE), :128] = left
        out_ref[part, pl.ds(at, TILE), 128:] = right

        @pl.when((local < WIN - PART_SLOTS) & (part > 0))
        def _():
            again = pl.multiple_of((PART_SLOTS + local) * TILE, TILE)
            out_ref[part - 1, pl.ds(again, TILE), :128] = left
            out_ref[part - 1, pl.ds(again, TILE), 128:] = right

        return carry

    lax.fori_loop(0, SLOTS, move, 0)


def arrive_sort(slots, incoming):
    return pl.pallas_call(
        arrive_kernel,
        grid_spec=pltpu.PrefetchScalarGridSpec(
            num_scalar_prefetch=1,
            grid=(1,),
            in_specs=[pl.BlockSpec(incoming.shape, lambda i, a: (0, 0, 0))],
            out_specs=pl.BlockSpec((PARTS, ROWS_W, PW), lambda i, a: (0, 0, 0)),
        ),
        out_shape=jax.ShapeDtypeStruct((PARTS, ROWS_W, PW), jnp.bfloat16),
        compiler_params=VMEM,
        name="arrive_sort",
    )(slots, incoming)


def block_kernel(meta_ref, x_ref, own_m, own_o, a_m, a_o, b_m, b_o, c_m1, c_m2, c_o1, c_o2, out_ref, sum_ref,
                 norm_ref, q_ref, k_ref, v_ref, att_ref, acc_ref, w_refs, sems):
    core = meta_ref[10]
    first = meta_ref[0]
    count = meta_ref[1]
    copies = []
    sources = ((own_m, None), (own_o, None), (a_m, None), (a_o, None), (b_m, None), (b_o, None), (c_m1, c_m2), (c_o1, c_o2))
    at = 0
    for n, (one, two) in enumerate(sources):
        if two is None:
            copies.append([pltpu.make_async_copy(one, w_refs.at[n], sems.at[at])])
            at += 1
        else:
            copies.append([
                pltpu.make_async_copy(one, w_refs.at[n, 0:2], sems.at[at]),
                pltpu.make_async_copy(two, w_refs.at[n, 2:4], sems.at[at + 1]),
            ])
            at += 2
    for group in copies:
        for copy in group:
            copy.start()

    chunk = 64

    def norm(i, carry):
        at = pl.multiple_of(i * chunk, chunk)
        rows = [x_ref[p, pl.ds(at, chunk), :].astype(jnp.float32) for p in range(PARTS)]
        mean = sum(jnp.sum(r, axis=-1, keepdims=True) for r in rows) * (1.0 / D)
        centred = [r - mean for r in rows]
        spread = sum(jnp.sum(r * r, axis=-1, keepdims=True) for r in centred) * (1.0 / D)
        scale = lax.rsqrt(spread + EPSILON)
        for p in range(PARTS):
            norm_ref[p // 2, pl.ds(at, chunk), (p % 2) * PW : (p % 2 + 1) * PW] = (centred[p] * scale).astype(jnp.bfloat16)
        return carry

    lax.fori_loop(0, ROWS_W // chunk, norm, 0)
    lane = lax.broadcasted_iota(jnp.int32, (IMG_ROWS, PW), 1)
    low = lax.broadcasted_iota(jnp.int32, (IMG_ROWS, 128), 1) < HD

    for g in range(PARTS):
        for copy in copies[2 * g] + copies[2 * g + 1]:
            copy.wait()
        mine = norm_ref[core]
        other = norm_ref[1 - core]
        for n, ref in enumerate((q_ref, k_ref, v_ref)):
            total = jnp.dot(mine, w_refs[2 * g, n], preferred_element_type=jnp.float32)
            total = total + jnp.dot(other, w_refs[2 * g + 1, n], preferred_element_type=jnp.float32)
            ref[...] = total.astype(jnp.bfloat16)

        def image(i, carry):
            row = pl.multiple_of(meta_ref[2 + i] * TILE, TILE)
            limit = (meta_ref[6 + i] - meta_ref[2 + i]) * TILE
            queries = q_ref[pl.ds(row, IMG_ROWS), :]
            keys = k_ref[pl.ds(row, IMG_ROWS), :]
            values = v_ref[pl.ds(row, IMG_ROWS), :]
            allowed = lane < limit
            parts = []
            for h in range(PW // HD):
                inside = (lane >= h * HD) & (lane < (h + 1) * HD)
                head_keys = jnp.where(inside, keys, jnp.zeros_like(keys))
                head_values = jnp.where(inside, values, jnp.ones_like(values))
                scores = lax.dot_general(queries, head_keys, (((1,), (1,)), ((), ())), preferred_element_type=jnp.float32)
                scores = jnp.where(allowed, scores, -1e30)
                peak = jnp.max(scores, axis=-1, keepdims=True)
                raised = jnp.exp((scores - peak) * HD ** (-0.5)).astype(jnp.bfloat16)
                mixed = jnp.dot(raised, head_values, preferred_element_type=jnp.float32)
                near, far = (mixed[:, :128], mixed[:, 128:]) if h < 2 else (mixed[:, 128:], mixed[:, :128])
                parts.append(near / far)
            for half in range(2):
                att_ref[half, pl.ds(row, IMG_ROWS), :] = jnp.where(low, parts[2 * half], parts[2 * half + 1]).astype(jnp.bfloat16)
            return carry

        lax.fori_loop(0, count, image, 0)
        att_mine = att_ref[core]
        att_other = att_ref[1 - core]
        for n in range(PARTS):
            rows = slice(n * 128, (n + 1) * 128)
            term = jnp.dot(att_mine, w_refs[2 * g, 3, rows, :], preferred_element_type=jnp.float32)
            term = term + jnp.dot(att_other, w_refs[2 * g + 1, 3, rows, :], preferred_element_type=jnp.float32)
            term = term.astype(jnp.bfloat16).astype(jnp.float32)
            if g == 0:
                acc_ref[n] = term
            else:
                acc_ref[n] += term

    begin = meta_ref[2] * TILE
    end = meta_ref[11] * TILE
    row_ids = lax.broadcasted_iota(jnp.int32, (ROWS_W, PW), 0)
    live = (row_ids >= begin) & (row_ids < end)
    image_ids = lax.broadcasted_iota(jnp.int32, (IMG, WIN), 0)
    tile_ids = lax.broadcasted_iota(jnp.int32, (IMG, WIN), 1)
    lengths = jnp.ones((IMG, PW), jnp.float32)
    pooled_ids = lax.broadcasted_iota(jnp.int32, (IMG, PW), 0)
    member = jnp.zeros((IMG, WIN), jnp.float32)
    for i in range(MAX_LOCAL):
        here = (image_ids == first + i) & (tile_ids >= meta_ref[2 + i]) & (tile_ids < meta_ref[6 + i])
        member = jnp.where(here, 1.0, member)
        rows_i = ((meta_ref[6 + i] - meta_ref[2 + i]) * TILE).astype(jnp.float32)
        lengths = jnp.where((pooled_ids == first + i) & (rows_i > 0), rows_i, lengths)
    for n in range(PARTS):
        result = jnp.where(live, x_ref[n].astype(jnp.float32) + acc_ref[n], 0.0)
        out_ref[n, :ROWS_W, :] = result.astype(jnp.bfloat16)
        tile_sums = jnp.sum(result.reshape(WIN, TILE, PW), axis=1)
        sums = jnp.dot(member, tile_sums, precision=lax.Precision.HIGHEST, preferred_element_type=jnp.float32)
        pooled = sums / lengths
        one = pooled.astype(jnp.bfloat16)
        rest = pooled - one.astype(jnp.float32)
        two = rest.astype(jnp.bfloat16)
        three = (rest - two.astype(jnp.float32)).astype(jnp.bfloat16)
        out_ref[n, ROWS_W : ROWS_W + IMG, :] = one
        out_ref[n, ROWS_W + IMG : ROWS_W + 2 * IMG, :] = two
        out_ref[n, ROWS_W + 2 * IMG : ROWS_W + 3 * IMG, :] = three
        sum_ref[0:1, n * PW : (n + 1) * PW] = jnp.sum(pooled, axis=0, keepdims=True)
    sum_ref[1:2, :] = jnp.full((1, D), count, jnp.int32).astype(jnp.float32)


def block(meta, x, weights):
    whole = lambda i, a: (0, 0, 0)
    return pl.pallas_call(
        block_kernel,
        grid_spec=pltpu.PrefetchScalarGridSpec(
            num_scalar_prefetch=1,
            grid=(1,),
            in_specs=[pl.BlockSpec(x.shape, whole)] + [pl.BlockSpec(memory_space=pl.ANY)] * len(weights),
            out_specs=[
                pl.BlockSpec((PARTS, ROWS_W + EXTRA, PW), whole),
                pl.BlockSpec((2, D), lambda i, a: (0, 0)),
            ],
            scratch_shapes=[
                pltpu.VMEM((2, ROWS_W, D // 2), jnp.bfloat16),
                pltpu.VMEM((ROWS_W, PW), jnp.bfloat16),
                pltpu.VMEM((ROWS_W, PW), jnp.bfloat16),
                pltpu.VMEM((ROWS_W, PW), jnp.bfloat16),
                pltpu.VMEM((2, ROWS_W, PW // 2), jnp.bfloat16),
                pltpu.VMEM((PARTS, ROWS_W, PW), jnp.float32),
                pltpu.VMEM((2 * PARTS, 4, D // 2, PW), jnp.bfloat16),
                pltpu.SemaphoreType.DMA((10,)),
            ],
        ),
        out_shape=[
            jax.ShapeDtypeStruct((PARTS, ROWS_W + EXTRA, PW), jnp.bfloat16),
            jax.ShapeDtypeStruct((2, D), jnp.float32),
        ],
        compiler_params=VMEM,
        name="block",
    )(meta, x, *weights)


def finish_kernel(in_ref, out_ref):
    size = PART_SLOTS * TILE
    halo = ROWS_W - size
    for p in range(PARTS):
        start = in_ref[p, :halo, :]
        if p:
            start = start + in_ref[p - 1, size:ROWS_W, :]
        out_ref[p * size : p * size + halo, :] = start
        out_ref[p * size + halo : (p + 1) * size, :] = in_ref[p, halo:size, :]


def finish(incoming):
    return pl.pallas_call(
        finish_kernel,
        out_shape=jax.ShapeDtypeStruct((SLOTS * TILE, PW), jnp.bfloat16),
        compiler_params=VMEM,
        name="finish",
    )(incoming)


def packed_weights(w_query, w_key, w_value, w_out):
    half = D // 2
    inner = jnp.stack([w_query, w_key, w_value]).reshape(3, 2, half, PW).transpose(1, 0, 2, 3)
    outer = w_out.reshape(2, PW // 2, PARTS, PW).transpose(0, 2, 1, 3).reshape(2, 1, half, PW)
    return jnp.concatenate([inner, outer], axis=1)


def on_device(patches, dest_owner, dest_slot, packed_image, w_query, w_key, w_value, w_out):
    senders = lax.axis_size("dp")
    splits = lax.axis_size("mp")
    mp = lax.axis_index("mp")
    core = lax.axis_index("dp") % 2
    up = [(i, (i + 1) % splits) for i in range(splits)]
    down = [(i, (i - 1) % splits) for i in range(splits)]
    swap = [(i, i ^ 1) for i in range(senders)]

    both = packed_weights(w_query, w_key, w_value, w_out)
    own_m = lax.dynamic_index_in_dim(both, core, 0, keepdims=False)
    own_o = lax.dynamic_index_in_dim(both, 1 - core, 0, keepdims=False)
    a_m = lax.ppermute(own_m, "mp", up)
    b_m = lax.ppermute(own_m, "mp", down)
    c_m1 = lax.ppermute(a_m[:2], "mp", up)
    c_m2 = lax.ppermute(b_m[2:], "mp", down)
    a_o = lax.ppermute(a_m, "dp", swap)
    b_o = lax.ppermute(b_m, "dp", swap)
    c_o1 = lax.ppermute(c_m1, "dp", swap)
    c_o2 = lax.ppermute(c_m2, "dp", swap)

    labels = jnp.arange(IMG, dtype=jnp.int32)
    lengths = jnp.sum((packed_image[None, :] == labels[:, None]).astype(jnp.int32), axis=1)
    starts = jnp.sum(((packed_image[None, :] >= 0) & (packed_image[None, :] < labels[:, None])).astype(jnp.int32), axis=1)
    present = lengths > 0
    window = mp * PART_SLOTS
    inside = present & (starts >= window) & (starts < window + PART_SLOTS)
    count = jnp.sum(inside.astype(jnp.int32))
    first = jnp.sum((present & (starts < window)).astype(jnp.int32))
    local = jnp.arange(MAX_LOCAL, dtype=jnp.int32)
    chosen = inside[None, :] & (labels[None, :] == first + local[:, None])
    begin = jnp.sum(jnp.where(chosen, starts[None, :] - window, 0), axis=1)
    end = jnp.sum(jnp.where(chosen, starts[None, :] + lengths[None, :] - window, 0), axis=1)
    meta = jnp.concatenate([jnp.stack([first, count]), begin, end, jnp.stack([core, jnp.max(end)])]).astype(jnp.int32)

    outgoing = send_pack(dest_owner, dest_slot, mp.reshape(1).astype(jnp.int32), patches, senders)
    incoming = lax.all_to_all(outgoing, "dp", split_axis=0, concat_axis=0, tiled=True)
    got_slot = incoming[:, 64:66, 0].astype(jnp.int32).reshape(SLOTS)
    windows = arrive_sort(got_slot, incoming)
    rows = lax.all_to_all(windows, "mp", split_axis=0, concat_axis=0, tiled=True)
    result, local_sum = block(meta, rows, (own_m, own_o, a_m, a_o, b_m, b_o, c_m1, c_m2, c_o1, c_o2))
    total = lax.psum(local_sum, ("dp", "mp"))
    back = lax.all_to_all(result, "mp", split_axis=0, concat_axis=0, tiled=True)
    packed_out = finish(back)
    pooled = jnp.sum(back[:, ROWS_W:, :].astype(jnp.float32).reshape(PARTS, 3, IMG, PW), axis=(0, 1))
    centre = lax.dynamic_slice_in_dim(total[0], mp * PW, PW) / total[1, 0]
    pooled_out = jnp.where(present[:, None], pooled - centre[None, :], 0.0).astype(jnp.bfloat16)
    return (packed_out, pooled_out)


def solution(mesh):
    in_specs = (
        P("dp", None),
        P("dp"),
        P("dp"),
        P("dp"),
        P(None, "mp"),
        P(None, "mp"),
        P(None, "mp"),
        P("mp", None),
    )
    out_specs = (P("dp", "mp"), P("dp", "mp"))
    return jax.shard_map(on_device, mesh=mesh, in_specs=in_specs, out_specs=out_specs, check_vma=False)
```

```python
import jax
import jax.numpy as jnp
from jax import lax
from jax.experimental import pallas as pl
from jax.experimental.pallas import tpu as pltpu
from jax.sharding import PartitionSpec as P

EPSILON = 1e-06
SLOTS = 128
TILE = 16
D = 1024
PARTS = 4
PW = D // PARTS
PART_SLOTS = SLOTS // PARTS
WIN = PART_SLOTS + 16
ROWS_W = WIN * TILE
IMG = 16
EXTRA = 3 * IMG
HD = 64
MAX_LOCAL = 4
PAY = 72
IMG_ROWS = 256
EXP_SCALE = HD ** (-0.5) * 1.4426950408889634
VMEM = pltpu.CompilerParams(vmem_limit_bytes=56 * 1024 * 1024)


def send_kernel(owner_ref, slot_ref, mp_ref, image_ref, patch_ref, out_ref, count_ref, place_ref):
    owners = out_ref.shape[0]

    def clear(o, carry):
        count_ref[o] = 0
        return carry

    lax.fori_loop(0, owners, clear, 0, unroll=8)

    def move(t, carry):
        o = owner_ref[t]
        r = count_ref[o]
        count_ref[o] = r + 1
        place_ref[2 * o + r] = slot_ref[t]
        rows = patch_ref[pl.ds(pl.multiple_of(t * TILE, TILE), TILE), :]
        base = pl.multiple_of(r * 2 * TILE, TILE)
        out_ref[o, pl.ds(base, TILE), :] = rows[:, :128]
        out_ref[o, pl.ds(base + TILE, TILE), :] = rows[:, 128:]
        return carry

    lax.fori_loop(0, SLOTS, move, 0, unroll=8)
    row = lax.broadcasted_iota(jnp.int32, (PAY - 64, 128), 0)
    images = jnp.max(image_ref[...], axis=1, keepdims=True) + 1
    images = jnp.broadcast_to(images, row.shape)

    def label(o, carry):
        value = jnp.where(row == 0, place_ref[2 * o], jnp.where(row == 1, place_ref[2 * o + 1], images))
        out_ref[o, 64:, :] = value.astype(jnp.float32).astype(jnp.bfloat16)
        return carry

    lax.fori_loop(0, owners, label, 0, unroll=8)


def send_pack(owner, slot, mp, image, patches, senders):
    return pl.pallas_call(
        send_kernel,
        grid_spec=pltpu.PrefetchScalarGridSpec(
            num_scalar_prefetch=3,
            grid=(1,),
            in_specs=[
                pl.BlockSpec((1, SLOTS), lambda i, a, b, m: (0, 0)),
                pl.BlockSpec((SLOTS * TILE, PW), lambda i, a, b, m: (0, m[0])),
            ],
            out_specs=pl.BlockSpec((senders, PAY, 128), lambda i, a, b, m: (0, 0, 0)),
            scratch_shapes=[pltpu.SMEM((senders,), jnp.int32), pltpu.SMEM((2 * senders,), jnp.int32)],
        ),
        out_shape=jax.ShapeDtypeStruct((senders, PAY, 128), jnp.bfloat16),
        compiler_params=VMEM,
        name="send_pack",
    )(owner, slot, mp, image, patches)


def arrive_kernel(mp_ref, in_ref, out0, out1, out2, out3, total_ref, sorted_ref, label_ref, slot_ref, sems):
    senders = in_ref.shape[0]
    row = lax.broadcasted_iota(jnp.int32, (8, 128), 0)
    lane = lax.broadcasted_iota(jnp.int32, (8, 128), 1)
    picked = jnp.zeros((8, 128), jnp.float32)
    total = jnp.zeros((8, 128), jnp.float32)
    for s in range(senders):
        marks = in_ref[s, 64:, :].astype(jnp.float32)
        picked = jnp.where((lane == 2 * s) | (lane == 2 * s + 1), marks, picked)
        total = total + marks
    odd = (lane & 1) == 1
    own = jnp.where(row == jnp.where(odd, 1, 0), picked, 0.0)
    label_ref[...] = jnp.broadcast_to(jnp.sum(own, axis=0, keepdims=True), (8, 128)).astype(jnp.int32)
    copy = pltpu.make_async_copy(label_ref, slot_ref, sems.at[4])
    copy.start()
    total_ref[...] = jnp.broadcast_to(jnp.sum(jnp.where(row == 2, total, 0.0), axis=0, keepdims=True), (8, 128))
    sorted_ref[SLOTS * TILE :, :] = jnp.zeros((ROWS_W - PART_SLOTS * TILE, PW), jnp.bfloat16)
    copy.wait()

    def move(s, carry):
        for r in range(2):
            at = pl.multiple_of(slot_ref[0, 2 * s + r] * TILE, TILE)
            sorted_ref[pl.ds(at, TILE), :128] = in_ref[s, 2 * r * TILE : (2 * r + 1) * TILE, :]
            sorted_ref[pl.ds(at, TILE), 128:] = in_ref[s, (2 * r + 1) * TILE : (2 * r + 2) * TILE, :]
        return carry

    lax.fori_loop(0, senders, move, 0, unroll=8)
    copies = []
    for d, out in enumerate((out0, out1, out2, out3)):
        part = (mp_ref[0] + d) % PARTS
        at = pl.multiple_of(part * PART_SLOTS * TILE, TILE)
        copies.append(pltpu.make_async_copy(sorted_ref.at[pl.ds(at, ROWS_W), :], out, sems.at[d]))
    for copy in copies:
        copy.start()
    for copy in copies:
        copy.wait()


def arrive_sort(mp, incoming):
    window = jax.ShapeDtypeStruct((ROWS_W, PW), jnp.bfloat16)
    return pl.pallas_call(
        arrive_kernel,
        grid_spec=pltpu.PrefetchScalarGridSpec(
            num_scalar_prefetch=1,
            grid=(1,),
            in_specs=[pl.BlockSpec(incoming.shape, lambda i, a: (0, 0, 0))],
            out_specs=[pl.BlockSpec(memory_space=pl.ANY)] * PARTS + [pl.BlockSpec((8, 128), lambda i, a: (0, 0))],
            scratch_shapes=[
                pltpu.VMEM((SLOTS * TILE + ROWS_W - PART_SLOTS * TILE, PW), jnp.bfloat16),
                pltpu.VMEM((8, 128), jnp.int32),
                pltpu.SMEM((8, 128), jnp.int32),
                pltpu.SemaphoreType.DMA((5,)),
            ],
        ),
        out_shape=[window] * PARTS + [jax.ShapeDtypeStruct((8, 128), jnp.float32)],
        compiler_params=VMEM,
        name="arrive_sort",
    )(mp, incoming)


def block_kernel(place_ref, image_ref, x0, x1, x2, x3, wq, wk, wv, wo, a0, a1, a0x, a1x, b0, b1, b0x, b1x, c0, c1, c0x, c1x,
                 out0, out1, out2, out3, sum_ref,
                 x_ref, norm_ref, q_ref, k_ref, v_ref, att_ref, w_refs, begin_ref, end_ref, xsem, wsem):
    part = place_ref[0]
    core = place_ref[1]
    x_copies = []
    for d, x in enumerate((x0, x1, x2, x3)):
        x_copies.append(pltpu.make_async_copy(x, x_ref.at[(part + PARTS - d) % PARTS], xsem.at[d]))
        x_copies[-1].start()
    copies = [[pltpu.make_async_copy(w, w_refs.at[0, n], wsem.at[n]) for n, w in enumerate((wq, wk, wv, wo))]]
    for g, (m0, m1, o0, o1) in enumerate(((a0, a1, a0x, a1x), (b0, b1, b0x, b1x), (c0, c1, c0x, c1x))):
        group = []
        for n, (w, place) in enumerate(((m0, 2 * core), (m1, 2 * core + 1), (o0, 2 - 2 * core), (o1, 3 - 2 * core))):
            group.append(pltpu.make_async_copy(w, w_refs.at[g + 1, place], wsem.at[4 * g + 4 + n]))
        copies.append(group)
    for group in copies:
        for copy in group:
            copy.start()

    window = part * PART_SLOTS
    for i in range(8):
        begin_ref[i] = 0
        end_ref[i] = 0

    def scan(l, carry):
        before, count, first, mine = carry
        t = window + l
        label = jnp.where(t < SLOTS, image_ref[jnp.minimum(t, SLOTS - 1)], -1)
        fresh = (label >= 0) & (label != before)
        starts = fresh & (l < PART_SLOTS)
        mine = jnp.where(fresh, jnp.where(starts, 1, 0), jnp.where(label >= 0, mine, 0))
        first = jnp.where(starts & (count == 0), label, first)
        count = count + jnp.where(starts, 1, 0)
        begin_ref[jnp.where(starts, count - 1, 7)] = l
        end_ref[jnp.where(mine == 1, count - 1, 7)] = l + 1
        return label, count, first, mine

    before = jnp.where(part > 0, image_ref[jnp.maximum(window - 1, 0)], -1)
    _, count, first, _ = lax.fori_loop(0, WIN, scan, (before, jnp.int32(0), jnp.int32(0), jnp.int32(0)), unroll=4)
    for copy in x_copies:
        copy.wait()

    chunk = 64

    def norm(i, carry):
        at = pl.multiple_of(i * chunk, chunk)
        rows = [x_ref[p, pl.ds(at, chunk), :].astype(jnp.float32) for p in range(PARTS)]
        mean = jnp.sum(rows[0] + rows[1] + rows[2] + rows[3], axis=-1, keepdims=True) * (1.0 / D)
        centred = [r - mean for r in rows]
        squares = [r * r for r in centred]
        spread = jnp.sum(squares[0] + squares[1] + squares[2] + squares[3], axis=-1, keepdims=True) * (1.0 / D)
        scale = lax.rsqrt(spread + EPSILON)
        for p in range(PARTS):
            norm_ref[pl.ds(at, chunk), p * PW : (p + 1) * PW] = (centred[p] * scale).astype(jnp.bfloat16)
        return carry

    lax.fori_loop(0, ROWS_W // chunk, norm, 0)
    lane = lax.broadcasted_iota(jnp.int32, (IMG_ROWS, PW), 1)
    upper = lax.broadcasted_iota(jnp.int32, (IMG_ROWS, 128), 1) + 128
    low = lax.broadcasted_iota(jnp.int32, (IMG_ROWS, 128), 1) < HD

    for g in range(PARTS):
        for copy in copies[g]:
            copy.wait()
        for n, ref in enumerate((q_ref, k_ref, v_ref)):
            ref[...] = jnp.dot(norm_ref[...], w_refs[g, n], preferred_element_type=jnp.float32).astype(jnp.bfloat16)

        def image(i, carry):
            row = pl.multiple_of(begin_ref[i] * TILE, TILE)
            limit = (end_ref[i] - begin_ref[i]) * TILE
            queries = q_ref[pl.ds(row, IMG_ROWS), :]
            keys = k_ref[pl.ds(row, IMG_ROWS), :]
            values = v_ref[pl.ds(row, IMG_ROWS), :]
            allowed = upper < limit
            nears, fars = [], []
            for h in range(PW // HD):
                inside = (lane >= h * HD) & (lane < (h + 1) * HD)
                head_keys = jnp.where(inside, keys, jnp.zeros_like(keys))
                head_values = jnp.where(inside, values, jnp.ones_like(values))
                scores = lax.dot_general(queries, head_keys, (((1,), (1,)), ((), ())), preferred_element_type=jnp.float32)
                always, maybe = scores[:, :128], jnp.where(allowed, scores[:, 128:], -1e30)
                peak = jnp.max(jnp.maximum(always, maybe), axis=-1, keepdims=True)
                raised = jnp.exp2((jnp.concatenate([always, maybe], axis=1) - peak) * EXP_SCALE).astype(jnp.bfloat16)
                mixed = jnp.dot(raised, head_values, preferred_element_type=jnp.float32)
                near, far = (mixed[:, :128], mixed[:, 128:]) if h < 2 else (mixed[:, 128:], mixed[:, :128])
                nears.append(near)
                fars.append(far)
            for half in range(2):
                top = jnp.where(low, nears[2 * half], nears[2 * half + 1])
                bottom = jnp.where(low, fars[2 * half], fars[2 * half + 1])
                att_ref[pl.ds(row, IMG_ROWS), g * PW + half * 128 : g * PW + (half + 1) * 128] = (top / bottom).astype(jnp.bfloat16)
            return carry

        lax.fori_loop(0, count, image, 0)

    start_row = begin_ref[0] * TILE
    end_row = end_ref[0]
    for i in range(1, MAX_LOCAL):
        end_row = jnp.maximum(end_row, end_ref[i])
    end_row = end_row * TILE
    row_ids = lax.broadcasted_iota(jnp.int32, (ROWS_W, PW), 0)
    live = (row_ids >= start_row) & (row_ids < end_row)
    image_ids = lax.broadcasted_iota(jnp.int32, (IMG, WIN), 0)
    tile_ids = lax.broadcasted_iota(jnp.int32, (IMG, WIN), 1)
    lengths = jnp.ones((IMG, PW), jnp.float32)
    pooled_ids = lax.broadcasted_iota(jnp.int32, (IMG, PW), 0)
    member = jnp.zeros((IMG, WIN), jnp.float32)
    for i in range(MAX_LOCAL):
        here = (image_ids == first + i) & (tile_ids >= begin_ref[i]) & (tile_ids < end_ref[i])
        member = jnp.where(here, 1.0, member)
        rows_i = ((end_ref[i] - begin_ref[i]) * TILE).astype(jnp.float32)
        lengths = jnp.where((pooled_ids == first + i) & (rows_i > 0), rows_i, lengths)
    for d, out in enumerate((out0, out1, out2, out3)):
        n = (part + d) % PARTS
        block_rows = pl.ds(pl.multiple_of(n * PW, PW), PW)
        mix = jnp.concatenate([w_refs[g, 3, block_rows, :] for g in range(PARTS)], axis=0)
        projected = jnp.dot(att_ref[...], mix, preferred_element_type=jnp.float32)
        result = jnp.where(live, x_ref[n].astype(jnp.float32) + projected, 0.0)
        out[:ROWS_W, :] = result.astype(jnp.bfloat16)
        tile_sums = jnp.sum(result.reshape(WIN, TILE, PW), axis=1)
        sums = jnp.dot(member, tile_sums, precision=lax.Precision.HIGHEST, preferred_element_type=jnp.float32)
        pooled = sums / lengths
        one = pooled.astype(jnp.bfloat16)
        rest = pooled - one.astype(jnp.float32)
        two = rest.astype(jnp.bfloat16)
        three = (rest - two.astype(jnp.float32)).astype(jnp.bfloat16)
        out[ROWS_W : ROWS_W + IMG, :] = one
        out[ROWS_W + IMG : ROWS_W + 2 * IMG, :] = two
        out[ROWS_W + 2 * IMG : ROWS_W + 3 * IMG, :] = three
        sum_ref[pl.ds(n, 1), :] = jnp.sum(pooled, axis=0, keepdims=True)


def block(place, image, xs, weights):
    outs = jax.ShapeDtypeStruct((ROWS_W + EXTRA, PW), jnp.bfloat16)
    whole = lambda i, a, b: (0, 0)
    wide = pltpu.VMEM((ROWS_W, PW), jnp.bfloat16)
    return pl.pallas_call(
        block_kernel,
        grid_spec=pltpu.PrefetchScalarGridSpec(
            num_scalar_prefetch=2,
            grid=(1,),
            in_specs=[pl.BlockSpec(memory_space=pl.ANY)] * (len(xs) + len(weights)),
            out_specs=[pl.BlockSpec((ROWS_W + EXTRA, PW), whole)] * PARTS + [pl.BlockSpec((PARTS, PW), whole)],
            scratch_shapes=[
                pltpu.VMEM((PARTS, ROWS_W, PW), jnp.bfloat16),
                pltpu.VMEM((ROWS_W, D), jnp.bfloat16),
                wide,
                wide,
                wide,
                pltpu.VMEM((ROWS_W, D), jnp.bfloat16),
                pltpu.VMEM((PARTS, 4, D, PW), jnp.bfloat16),
                pltpu.SMEM((8,), jnp.int32),
                pltpu.SMEM((8,), jnp.int32),
                pltpu.SemaphoreType.DMA((PARTS,)),
                pltpu.SemaphoreType.DMA((4 * PARTS,)),
            ],
        ),
        out_shape=[outs] * PARTS + [jax.ShapeDtypeStruct((PARTS, PW), jnp.float32)],
        compiler_params=VMEM,
        name="block",
    )(place, image, *xs, *weights)


def finish_kernel(place_ref, r0, r1, r2, r3, out_ref, pooled_ref, in_ref, out_vmem, sems, out_sems):
    size = PART_SLOTS * TILE
    halo = ROWS_W - size
    part = place_ref[0]
    copies = []
    for d, r in enumerate((r0, r1, r2, r3)):
        copies.append(pltpu.make_async_copy(r, in_ref.at[(part + PARTS - d) % PARTS], sems.at[d]))
    for copy in copies:
        copy.start()
    for copy in copies:
        copy.wait()
    writes = []
    for p in range(PARTS):
        start = in_ref[p, :halo, :]
        if p:
            start = start + in_ref[p - 1, size:ROWS_W, :]
        out_vmem[p * size : p * size + halo, :] = start
        out_vmem[p * size + halo : (p + 1) * size, :] = in_ref[p, halo:size, :]
        rows = pl.ds(p * size, size)
        writes.append(pltpu.make_async_copy(out_vmem.at[rows, :], out_ref.at[rows, :], out_sems.at[p]))
        writes[-1].start()
    pooled = jnp.zeros((IMG, PW), jnp.float32)
    for p in range(PARTS):
        for n in range(3):
            pooled = pooled + in_ref[p, ROWS_W + n * IMG : ROWS_W + (n + 1) * IMG, :].astype(jnp.float32)
    pooled_ref[...] = pooled
    for write in writes:
        write.wait()


def finish(place, received):
    return pl.pallas_call(
        finish_kernel,
        grid_spec=pltpu.PrefetchScalarGridSpec(
            num_scalar_prefetch=1,
            grid=(1,),
            in_specs=[pl.BlockSpec(memory_space=pl.ANY)] * PARTS,
            out_specs=[pl.BlockSpec(memory_space=pl.ANY), pl.BlockSpec((IMG, PW), lambda i, a: (0, 0))],
            scratch_shapes=[
                pltpu.VMEM((PARTS, ROWS_W + EXTRA, PW), jnp.bfloat16),
                pltpu.VMEM((SLOTS * TILE, PW), jnp.bfloat16),
                pltpu.SemaphoreType.DMA((PARTS,)),
                pltpu.SemaphoreType.DMA((PARTS,)),
            ],
        ),
        out_shape=[
            jax.ShapeDtypeStruct((SLOTS * TILE, PW), jnp.bfloat16),
            jax.ShapeDtypeStruct((IMG, PW), jnp.float32),
        ],
        compiler_params=VMEM,
        name="finish",
    )(place, *received)


def whole_block(patches, dest_owner, dest_slot, packed_image, w_query, w_key, w_value, w_out):
    senders = lax.axis_size("dp")
    splits = lax.axis_size("mp")
    mp = lax.axis_index("mp").astype(jnp.int32)
    core = (lax.axis_index("dp") % 2).astype(jnp.int32)
    place = jnp.stack([mp, core])
    shift = lambda d: [(i, (i + d) % splits) for i in range(splits)]
    swap = [(i, i ^ 1) for i in range(senders)]

    out_blocks = w_out.reshape(PW, PARTS, PW).transpose(1, 0, 2).reshape(D, PW)
    s0 = jnp.where(core == 0, w_query, w_value)
    s1 = jnp.where(core == 0, w_key, out_blocks)
    a0, a1 = (lax.ppermute(s, "mp", shift(1)) for s in (s0, s1))
    b0, b1 = (lax.ppermute(s, "mp", shift(-1)) for s in (s0, s1))
    c0 = lax.ppermute(a0, "mp", shift(1))
    c1 = lax.ppermute(b1, "mp", shift(-1))
    a0x, a1x, b0x, b1x, c0x, c1x = (lax.ppermute(w, "dp", swap) for w in (a0, a1, b0, b1, c0, c1))
    weights = (w_query, w_key, w_value, out_blocks, a0, a1, a0x, a1x, b0, b1, b0x, b1x, c0, c1, c0x, c1x)

    outgoing = send_pack(dest_owner, dest_slot, place[:1], packed_image.reshape(1, SLOTS), patches, senders)
    incoming = lax.all_to_all(outgoing, "dp", split_axis=0, concat_axis=0, tiled=True)
    *windows, number = arrive_sort(place[:1], incoming)
    rows = [windows[0]] + [lax.ppermute(windows[d], "mp", shift(d)) for d in (1, 2, 3)]
    *results, local_sum = block(place, packed_image, rows, weights)
    received = [results[0]] + [lax.ppermute(results[d], "mp", shift(d)) for d in (1, 2, 3)]
    spread = jnp.broadcast_to(local_sum.reshape(1, PARTS, 2, PW // 2), (senders, PARTS, 2, PW // 2))
    gathered = lax.all_to_all(
        spread.reshape(senders * PARTS, 2, PW // 2), ("dp", "mp"), split_axis=0, concat_axis=0, tiled=True
    )
    packed_out, pooled = finish(place[:1], received)
    centre = (jnp.sum(gathered, axis=0) / number[0, 0]).reshape(1, PW)
    present = jnp.any(packed_image[None, :] == jnp.arange(IMG, dtype=jnp.int32)[:, None], axis=1, keepdims=True)
    pooled_out = jnp.where(present, pooled - centre, 0.0).astype(jnp.bfloat16)
    return (packed_out, pooled_out)


def solution(mesh):
    in_specs = (
        P("dp", None),
        P("dp"),
        P("dp"),
        P("dp"),
        P(None, "mp"),
        P(None, "mp"),
        P(None, "mp"),
        P("mp", None),
    )
    out_specs = (P("dp", "mp"), P("dp", "mp"))
    return jax.shard_map(whole_block, mesh=mesh, in_specs=in_specs, out_specs=out_specs, check_vma=False)
```

```python
import jax
import jax.numpy as jnp
from jax import lax
from jax.experimental import pallas as pl
from jax.experimental.pallas import tpu as pltpu
from jax.sharding import PartitionSpec as P

EPSILON = 1e-06
SLOTS = 128
TILE = 16
D = 1024
PARTS = 4
PW = D // PARTS
PART_SLOTS = SLOTS // PARTS
WIN = PART_SLOTS + 16
ROWS_W = WIN * TILE
IMG = 16
EXTRA = 3 * IMG
HD = 64
MAX_LOCAL = 4
PAY = 72
IMG_ROWS = 256
EXP_SCALE = HD ** (-0.5) * 1.4426950408889634
VMEM = pltpu.CompilerParams(vmem_limit_bytes=56 * 1024 * 1024)


def send_kernel(owner_ref, slot_ref, mp_ref, image_ref, patch_ref, wq, wk, wv, wo, out_ref, s0, s1, count_ref, place_ref, sems):
    owners = out_ref.shape[0]
    core = mp_ref[1]
    even = [pltpu.make_async_copy(wq, s0, sems.at[0]), pltpu.make_async_copy(wk, s1, sems.at[1])]
    odd = [pltpu.make_async_copy(wv, s0, sems.at[0])]
    for n in range(PARTS):
        block_rows = pl.ds(n * PW, PW)
        odd.append(pltpu.make_async_copy(wo.at[:, block_rows], s1.at[block_rows, :], sems.at[1 + n]))

    @pl.when(core == 0)
    def _():
        for copy in even:
            copy.start()

    @pl.when(core != 0)
    def _():
        for copy in odd:
            copy.start()

    def clear(o, carry):
        count_ref[o] = 0
        return carry

    lax.fori_loop(0, owners, clear, 0, unroll=8)

    def move(t, carry):
        o = owner_ref[t]
        r = count_ref[o]
        count_ref[o] = r + 1
        place_ref[2 * o + r] = slot_ref[t]
        rows = patch_ref[pl.ds(pl.multiple_of(t * TILE, TILE), TILE), :]
        base = pl.multiple_of(r * 2 * TILE, TILE)
        out_ref[o, pl.ds(base, TILE), :] = rows[:, :128]
        out_ref[o, pl.ds(base + TILE, TILE), :] = rows[:, 128:]
        return carry

    lax.fori_loop(0, SLOTS, move, 0, unroll=8)
    row = lax.broadcasted_iota(jnp.int32, (PAY - 64, 128), 0)
    images = jnp.max(image_ref[...], axis=1, keepdims=True) + 1
    images = jnp.broadcast_to(images, row.shape)

    def label(o, carry):
        value = jnp.where(row == 0, place_ref[2 * o], jnp.where(row == 1, place_ref[2 * o + 1], images))
        out_ref[o, 64:, :] = value.astype(jnp.float32).astype(jnp.bfloat16)
        return carry

    lax.fori_loop(0, owners, label, 0, unroll=8)

    @pl.when(core == 0)
    def _():
        for copy in even:
            copy.wait()

    @pl.when(core != 0)
    def _():
        for copy in odd:
            copy.wait()


def send_pack(owner, slot, place, image, patches, weights, senders):
    return pl.pallas_call(
        send_kernel,
        grid_spec=pltpu.PrefetchScalarGridSpec(
            num_scalar_prefetch=3,
            grid=(1,),
            in_specs=[
                pl.BlockSpec((1, SLOTS), lambda i, a, b, m: (0, 0)),
                pl.BlockSpec((SLOTS * TILE, PW), lambda i, a, b, m: (0, m[0])),
            ]
            + [pl.BlockSpec(memory_space=pl.ANY)] * 4,
            out_specs=[pl.BlockSpec((senders, PAY, 128), lambda i, a, b, m: (0, 0, 0))]
            + [pl.BlockSpec(memory_space=pl.ANY)] * 2,
            scratch_shapes=[
                pltpu.SMEM((senders,), jnp.int32),
                pltpu.SMEM((2 * senders,), jnp.int32),
                pltpu.SemaphoreType.DMA((1 + PARTS,)),
            ],
        ),
        out_shape=[jax.ShapeDtypeStruct((senders, PAY, 128), jnp.bfloat16)]
        + [jax.ShapeDtypeStruct((D, PW), jnp.bfloat16)] * 2,
        compiler_params=VMEM,
        name="send_pack",
    )(owner, slot, place, image, patches, *weights)


def arrive_kernel(mp_ref, in_ref, out0, out1, out2, out3, total_ref, sorted_ref, label_ref, slot_ref, sems):
    senders = in_ref.shape[0]
    row = lax.broadcasted_iota(jnp.int32, (8, 128), 0)
    lane = lax.broadcasted_iota(jnp.int32, (8, 128), 1)
    picked = jnp.zeros((8, 128), jnp.float32)
    total = jnp.zeros((8, 128), jnp.float32)
    for s in range(senders):
        marks = in_ref[s, 64:, :].astype(jnp.float32)
        picked = jnp.where((lane == 2 * s) | (lane == 2 * s + 1), marks, picked)
        total = total + marks
    odd = (lane & 1) == 1
    own = jnp.where(row == jnp.where(odd, 1, 0), picked, 0.0)
    label_ref[...] = jnp.broadcast_to(jnp.sum(own, axis=0, keepdims=True), (8, 128)).astype(jnp.int32)
    copy = pltpu.make_async_copy(label_ref, slot_ref, sems.at[4])
    copy.start()
    total_ref[...] = jnp.broadcast_to(jnp.sum(jnp.where(row == 2, total, 0.0), axis=0, keepdims=True), (8, 128))
    sorted_ref[SLOTS * TILE :, :] = jnp.zeros((ROWS_W - PART_SLOTS * TILE, PW), jnp.bfloat16)
    copy.wait()

    def move(s, carry):
        for r in range(2):
            at = pl.multiple_of(slot_ref[0, 2 * s + r] * TILE, TILE)
            sorted_ref[pl.ds(at, TILE), :128] = in_ref[s, 2 * r * TILE : (2 * r + 1) * TILE, :]
            sorted_ref[pl.ds(at, TILE), 128:] = in_ref[s, (2 * r + 1) * TILE : (2 * r + 2) * TILE, :]
        return carry

    lax.fori_loop(0, senders, move, 0, unroll=8)
    copies = []
    for d, out in enumerate((out0, out1, out2, out3)):
        part = (mp_ref[0] + d) % PARTS
        at = pl.multiple_of(part * PART_SLOTS * TILE, TILE)
        copies.append(pltpu.make_async_copy(sorted_ref.at[pl.ds(at, ROWS_W), :], out, sems.at[d]))
    for copy in copies:
        copy.start()
    for copy in copies:
        copy.wait()


def arrive_sort(mp, incoming):
    window = jax.ShapeDtypeStruct((ROWS_W, PW), jnp.bfloat16)
    return pl.pallas_call(
        arrive_kernel,
        grid_spec=pltpu.PrefetchScalarGridSpec(
            num_scalar_prefetch=1,
            grid=(1,),
            in_specs=[pl.BlockSpec(incoming.shape, lambda i, a: (0, 0, 0))],
            out_specs=[pl.BlockSpec(memory_space=pl.ANY)] * PARTS + [pl.BlockSpec((8, 128), lambda i, a: (0, 0))],
            scratch_shapes=[
                pltpu.VMEM((SLOTS * TILE + ROWS_W - PART_SLOTS * TILE, PW), jnp.bfloat16),
                pltpu.VMEM((8, 128), jnp.int32),
                pltpu.SMEM((8, 128), jnp.int32),
                pltpu.SemaphoreType.DMA((5,)),
            ],
        ),
        out_shape=[window] * PARTS + [jax.ShapeDtypeStruct((8, 128), jnp.float32)],
        compiler_params=VMEM,
        name="arrive_sort",
    )(mp, incoming)


def block_kernel(place_ref, image_ref, x0, x1, x2, x3, wq, wk, wv, wo, a0, a1, a0x, a1x, b0, b1, b0x, b1x, c0, c1, c0x, c1x,
                 out0, out1, out2, out3, sum0, sum1, sum2, sum3,
                 x_ref, norm_ref, q_ref, k_ref, v_ref, att_ref, w_refs, begin_ref, end_ref, xsem, wsem):
    part = place_ref[0]
    core = place_ref[1]
    x_copies = []
    for d, x in enumerate((x0, x1, x2, x3)):
        x_copies.append(pltpu.make_async_copy(x, x_ref.at[(part + PARTS - d) % PARTS], xsem.at[d]))
        x_copies[-1].start()
    copies = [[pltpu.make_async_copy(w, w_refs.at[0, n], wsem.at[n]) for n, w in enumerate((wq, wk, wv))]]
    for n in range(PARTS):
        block_rows = pl.ds(n * PW, PW)
        copies[0].append(pltpu.make_async_copy(wo.at[:, block_rows], w_refs.at[0, 3, block_rows, :], wsem.at[4 * PARTS - 1 + n]))
    for g, (m0, m1, o0, o1) in enumerate(((a0, a1, a0x, a1x), (b0, b1, b0x, b1x), (c0, c1, c0x, c1x))):
        group = []
        for n, (w, place) in enumerate(((m0, 2 * core), (m1, 2 * core + 1), (o0, 2 - 2 * core), (o1, 3 - 2 * core))):
            group.append(pltpu.make_async_copy(w, w_refs.at[g + 1, place], wsem.at[4 * g + 3 + n]))
        copies.append(group)
    for group in copies:
        for copy in group:
            copy.start()

    window = part * PART_SLOTS
    for i in range(8):
        begin_ref[i] = 0
        end_ref[i] = 0

    def scan(l, carry):
        before, count, first, mine = carry
        t = window + l
        label = jnp.where(t < SLOTS, image_ref[jnp.minimum(t, SLOTS - 1)], -1)
        fresh = (label >= 0) & (label != before)
        starts = fresh & (l < PART_SLOTS)
        mine = jnp.where(fresh, jnp.where(starts, 1, 0), jnp.where(label >= 0, mine, 0))
        first = jnp.where(starts & (count == 0), label, first)
        count = count + jnp.where(starts, 1, 0)
        begin_ref[jnp.where(starts, count - 1, 7)] = l
        end_ref[jnp.where(mine == 1, count - 1, 7)] = l + 1
        return label, count, first, mine

    before = jnp.where(part > 0, image_ref[jnp.maximum(window - 1, 0)], -1)
    _, count, first, _ = lax.fori_loop(0, WIN, scan, (before, jnp.int32(0), jnp.int32(0), jnp.int32(0)), unroll=4)
    for copy in x_copies:
        copy.wait()

    chunk = 128

    def norm(i, carry):
        at = pl.multiple_of(i * chunk, chunk)
        rows = [x_ref[p, pl.ds(at, chunk), :].astype(jnp.float32) for p in range(PARTS)]
        mean = jnp.sum(rows[0] + rows[1] + rows[2] + rows[3], axis=-1, keepdims=True) * (1.0 / D)
        centred = [r - mean for r in rows]
        squares = [r * r for r in centred]
        spread = jnp.sum(squares[0] + squares[1] + squares[2] + squares[3], axis=-1, keepdims=True) * (1.0 / D)
        scale = lax.rsqrt(spread + EPSILON)
        for p in range(PARTS):
            norm_ref[pl.ds(at, chunk), p * PW : (p + 1) * PW] = (centred[p] * scale).astype(jnp.bfloat16)
        return carry

    lax.fori_loop(0, ROWS_W // chunk, norm, 0)
    lane = lax.broadcasted_iota(jnp.int32, (IMG_ROWS, PW), 1)
    upper = lax.broadcasted_iota(jnp.int32, (IMG_ROWS, 128), 1) + 128
    low = lax.broadcasted_iota(jnp.int32, (IMG_ROWS, 128), 1) < HD

    for g in range(PARTS):
        for copy in copies[g]:
            copy.wait()
        for n, ref in enumerate((q_ref, k_ref, v_ref)):
            ref[...] = jnp.dot(norm_ref[...], w_refs[g, n], preferred_element_type=jnp.float32).astype(jnp.bfloat16)

        def image(i, carry):
            row = pl.multiple_of(begin_ref[i] * TILE, TILE)
            limit = (end_ref[i] - begin_ref[i]) * TILE

            def mix(size):
                window = pl.ds(row, size)
                queries = q_ref[window, :]
                keys = k_ref[window, :]
                values = v_ref[window, :]
                allowed = lax.broadcasted_iota(jnp.int32, (size, size - 128), 1) + 128 < limit
                lane = lax.broadcasted_iota(jnp.int32, (size, PW), 1)
                low = lax.broadcasted_iota(jnp.int32, (size, 128), 1) < HD
                heads = range(PW // HD)
                inside = [(lane >= h * HD) & (lane < (h + 1) * HD) for h in heads]
                nears, fars = [], []
                scores = [
                    lax.dot_general(queries, jnp.where(inside[h], keys, jnp.zeros_like(keys)), (((1,), (1,)), ((), ())), preferred_element_type=jnp.float32)
                    for h in heads
                ]
                raised = []
                for h in heads:
                    always, maybe = scores[h][:, :128], jnp.where(allowed, scores[h][:, 128:], -1e30)
                    peak = jnp.maximum(jnp.max(always, axis=-1, keepdims=True), jnp.max(maybe, axis=-1, keepdims=True))
                    raised.append(jnp.exp2((jnp.concatenate([always, maybe], axis=1) - peak) * EXP_SCALE).astype(jnp.bfloat16))
                for h in heads:
                    mixed = jnp.dot(raised[h], jnp.where(inside[h], values, jnp.ones_like(values)), preferred_element_type=jnp.float32)
                    near, far = (mixed[:, :128], mixed[:, 128:]) if h < 2 else (mixed[:, 128:], mixed[:, :128])
                    nears.append(near)
                    fars.append(far)
                for half in range(2):
                    top = jnp.where(low, nears[2 * half], nears[2 * half + 1])
                    bottom = jnp.where(low, fars[2 * half], fars[2 * half + 1])
                    att_ref[window, g * PW + half * 128 : g * PW + (half + 1) * 128] = (top / bottom).astype(jnp.bfloat16)

            @pl.when(limit <= 192)
            def _():
                mix(192)

            @pl.when(limit > 192)
            def _():
                mix(256)

            return carry

        lax.fori_loop(0, count, image, 0)

    start_row = begin_ref[0] * TILE
    end_row = end_ref[0]
    for i in range(1, MAX_LOCAL):
        end_row = jnp.maximum(end_row, end_ref[i])
    end_row = end_row * TILE
    row_ids = lax.broadcasted_iota(jnp.int32, (ROWS_W, PW), 0)
    live = (row_ids >= start_row) & (row_ids < end_row)
    tile_ids = lax.broadcasted_iota(jnp.int32, (WIN, 8, PW), 0)
    pooled_ids = lax.broadcasted_iota(jnp.int32, (IMG, PW), 0)
    lengths = jnp.ones((IMG, PW), jnp.float32)
    tiles = []
    for i in range(MAX_LOCAL):
        tiles.append((tile_ids >= begin_ref[i]) & (tile_ids < end_ref[i]))
        rows_i = ((end_ref[i] - begin_ref[i]) * TILE).astype(jnp.float32)
        lengths = jnp.where((pooled_ids == first + i) & (rows_i > 0), rows_i, lengths)
    for d, (out, sum_ref) in enumerate(((out0, sum0), (out1, sum1), (out2, sum2), (out3, sum3))):
        n = (part + d) % PARTS
        block_rows = pl.ds(pl.multiple_of(n * PW, PW), PW)
        mix = jnp.concatenate([w_refs[g, 3, block_rows, :] for g in range(PARTS)], axis=0)
        projected = jnp.dot(att_ref[...], mix, preferred_element_type=jnp.float32)
        result = jnp.where(live, x_ref[n].astype(jnp.float32) + projected, 0.0)
        out[:ROWS_W, :] = result.astype(jnp.bfloat16)
        pairs = result.reshape(WIN, 2, 8, PW)
        pairs = pairs[:, 0] + pairs[:, 1]
        sums = jnp.zeros((IMG, PW), jnp.float32)
        for i in range(MAX_LOCAL):
            held = jnp.sum(jnp.where(tiles[i], pairs, 0.0), axis=0)
            sums = jnp.where(pooled_ids == first + i, jnp.sum(held, axis=0, keepdims=True), sums)
        pooled = sums / lengths
        one = pooled.astype(jnp.bfloat16)
        rest = pooled - one.astype(jnp.float32)
        two = rest.astype(jnp.bfloat16)
        three = (rest - two.astype(jnp.float32)).astype(jnp.bfloat16)
        out[ROWS_W : ROWS_W + IMG, :] = one
        out[ROWS_W + IMG : ROWS_W + 2 * IMG, :] = two
        out[ROWS_W + 2 * IMG : ROWS_W + 3 * IMG, :] = three
        sum_ref[...] = jnp.sum(pooled, axis=0, keepdims=True)


def block(place, image, xs, weights):
    outs = jax.ShapeDtypeStruct((ROWS_W + EXTRA, PW), jnp.bfloat16)
    whole = lambda i, a, b: (0, 0)
    wide = pltpu.VMEM((ROWS_W, PW), jnp.bfloat16)
    return pl.pallas_call(
        block_kernel,
        grid_spec=pltpu.PrefetchScalarGridSpec(
            num_scalar_prefetch=2,
            grid=(1,),
            in_specs=[pl.BlockSpec(memory_space=pl.ANY)] * (len(xs) + len(weights)),
            out_specs=[pl.BlockSpec((ROWS_W + EXTRA, PW), whole)] * PARTS + [pl.BlockSpec((1, PW), whole)] * PARTS,
            scratch_shapes=[
                pltpu.VMEM((PARTS, ROWS_W, PW), jnp.bfloat16),
                pltpu.VMEM((ROWS_W, D), jnp.bfloat16),
                wide,
                wide,
                wide,
                pltpu.VMEM((ROWS_W, D), jnp.bfloat16),
                pltpu.VMEM((PARTS, 4, D, PW), jnp.bfloat16),
                pltpu.SMEM((8,), jnp.int32),
                pltpu.SMEM((8,), jnp.int32),
                pltpu.SemaphoreType.DMA((PARTS,)),
                pltpu.SemaphoreType.DMA((5 * PARTS - 1,)),
            ],
        ),
        out_shape=[outs] * PARTS + [jax.ShapeDtypeStruct((1, PW), jnp.float32)] * PARTS,
        compiler_params=VMEM,
        name="block",
    )(place, image, *xs, *weights)


def finish_kernel(place_ref, r0, r1, r2, r3, out_ref, pooled_ref, in_ref, out_vmem, sems, out_sems):
    size = PART_SLOTS * TILE
    halo = ROWS_W - size
    part = place_ref[0]
    copies = []
    for d, r in enumerate((r0, r1, r2, r3)):
        copies.append(pltpu.make_async_copy(r, in_ref.at[(part + PARTS - d) % PARTS], sems.at[d]))
    for copy in copies:
        copy.start()
    for copy in copies:
        copy.wait()
    writes = []
    for p in range(PARTS):
        start = in_ref[p, :halo, :]
        if p:
            start = start + in_ref[p - 1, size:ROWS_W, :]
        out_vmem[p * size : p * size + halo, :] = start
        out_vmem[p * size + halo : (p + 1) * size, :] = in_ref[p, halo:size, :]
        rows = pl.ds(p * size, size)
        writes.append(pltpu.make_async_copy(out_vmem.at[rows, :], out_ref.at[rows, :], out_sems.at[p]))
        writes[-1].start()
    pooled = jnp.zeros((IMG, PW), jnp.float32)
    for p in range(PARTS):
        for n in range(3):
            pooled = pooled + in_ref[p, ROWS_W + n * IMG : ROWS_W + (n + 1) * IMG, :].astype(jnp.float32)
    pooled_ref[...] = pooled
    for write in writes:
        write.wait()


def finish(place, received):
    return pl.pallas_call(
        finish_kernel,
        grid_spec=pltpu.PrefetchScalarGridSpec(
            num_scalar_prefetch=1,
            grid=(1,),
            in_specs=[pl.BlockSpec(memory_space=pl.ANY)] * PARTS,
            out_specs=[pl.BlockSpec(memory_space=pl.ANY), pl.BlockSpec((IMG, PW), lambda i, a: (0, 0))],
            scratch_shapes=[
                pltpu.VMEM((PARTS, ROWS_W + EXTRA, PW), jnp.bfloat16),
                pltpu.VMEM((SLOTS * TILE, PW), jnp.bfloat16),
                pltpu.SemaphoreType.DMA((PARTS,)),
                pltpu.SemaphoreType.DMA((PARTS,)),
            ],
        ),
        out_shape=[
            jax.ShapeDtypeStruct((SLOTS * TILE, PW), jnp.bfloat16),
            jax.ShapeDtypeStruct((IMG, PW), jnp.float32),
        ],
        compiler_params=VMEM,
        name="finish",
    )(place, *received)


def pool_kernel(sums_ref, number_ref, pooled_ref, image_ref, out_ref):
    total = jnp.sum(sums_ref[...], axis=0)
    centre = jnp.concatenate([total[0:1], total[1:2]], axis=1) / number_ref[0:1, 0:1]
    slots = lax.broadcasted_iota(jnp.int32, (IMG, SLOTS), 0) == image_ref[...]
    present = jnp.max(jnp.where(slots, 1.0, 0.0), axis=1, keepdims=True) > 0.5
    out_ref[...] = jnp.where(present, pooled_ref[...] - centre, 0.0).astype(jnp.bfloat16)


def pool(sums, number, pooled, image):
    return pl.pallas_call(
        pool_kernel,
        out_shape=jax.ShapeDtypeStruct((IMG, PW), jnp.bfloat16),
        name="pool",
    )(sums, number, pooled, image)


def whole_block(patches, dest_owner, dest_slot, packed_image, w_query, w_key, w_value, w_out):
    senders = lax.axis_size("dp")
    splits = lax.axis_size("mp")
    mp = lax.axis_index("mp").astype(jnp.int32)
    core = (lax.axis_index("dp") % 2).astype(jnp.int32)
    place = jnp.stack([mp, core])
    shift = lambda d: [(i, (i + d) % splits) for i in range(splits)]
    swap = [(i, i ^ 1) for i in range(senders)]

    own = (w_query, w_key, w_value, w_out)
    image = packed_image.reshape(1, SLOTS)
    outgoing, s0, s1 = send_pack(dest_owner, dest_slot, place, image, patches, own, senders)
    a0, a1 = (lax.ppermute(s, "mp", shift(1)) for s in (s0, s1))
    b0, b1 = (lax.ppermute(s, "mp", shift(-1)) for s in (s0, s1))
    c0 = lax.ppermute(a0, "mp", shift(1))
    c1 = lax.ppermute(b1, "mp", shift(-1))
    a0x, a1x, b0x, b1x, c0x, c1x = (lax.ppermute(w, "dp", swap) for w in (a0, a1, b0, b1, c0, c1))
    weights = own + (a0, a1, a0x, a1x, b0, b1, b0x, b1x, c0, c1, c0x, c1x)

    incoming = lax.all_to_all(outgoing, "dp", split_axis=0, concat_axis=0, tiled=True)
    *windows, number = arrive_sort(place[:1], incoming)
    rows = [windows[0]] + [lax.ppermute(windows[d], "mp", shift(d)) for d in (1, 2, 3)]
    outcome = block(place, packed_image, rows, weights)
    results, sums = outcome[:PARTS], outcome[PARTS:]
    total = sums[0] + sum(lax.ppermute(sums[d], "mp", shift(d)) for d in (1, 2, 3))
    received = [results[0]] + [lax.ppermute(results[d], "mp", shift(d)) for d in (1, 2, 3)]
    spread = jnp.broadcast_to(total.reshape(1, 2, PW // 2), (senders, 2, PW // 2))
    gathered = lax.all_to_all(spread, "dp", split_axis=0, concat_axis=0, tiled=True)
    packed_out, pooled = finish(place[:1], received)
    pooled_out = pool(gathered, number, pooled, image)
    return (packed_out, pooled_out)


def solution(mesh):
    in_specs = (
        P("dp", None),
        P("dp"),
        P("dp"),
        P("dp"),
        P(None, "mp"),
        P(None, "mp"),
        P(None, "mp"),
        P("mp", None),
    )
    out_specs = (P("dp", "mp"), P("dp", "mp"))
    return jax.shard_map(whole_block, mesh=mesh, in_specs=in_specs, out_specs=out_specs, check_vma=False)
```

```python
import jax
import jax.numpy as jnp
from jax import lax
from jax.experimental import pallas as pl
from jax.experimental.pallas import tpu as pltpu
from jax.sharding import PartitionSpec as P

EPSILON = 1e-06
SLOTS = 128
TILE = 16
D = 1024
PARTS = 4
PW = D // PARTS
PART_SLOTS = SLOTS // PARTS
WIN = PART_SLOTS + 16
ROWS_W = WIN * TILE
IMG = 16
EXTRA = 3 * IMG
HD = 64
MAX_LOCAL = 4
PAY = 72
IMG_ROWS = 256
EXP_SCALE = HD ** (-0.5) * 1.4426950408889634
VMEM = pltpu.CompilerParams(vmem_limit_bytes=56 * 1024 * 1024)


def send_kernel(owner_ref, slot_ref, mp_ref, image_ref, patch_ref, wq, wk, wv, wo, out_ref, s0, s1, count_ref, place_ref, sems):
    owners = out_ref.shape[0]
    core = mp_ref[1]
    even = [pltpu.make_async_copy(wq, s0, sems.at[0]), pltpu.make_async_copy(wk, s1, sems.at[1])]
    odd = [pltpu.make_async_copy(wv, s0, sems.at[0])]
    for n in range(PARTS):
        block_rows = pl.ds(n * PW, PW)
        odd.append(pltpu.make_async_copy(wo.at[:, block_rows], s1.at[block_rows, :], sems.at[1 + n]))

    @pl.when(core == 0)
    def _():
        for copy in even:
            copy.start()

    @pl.when(core != 0)
    def _():
        for copy in odd:
            copy.start()

    def clear(o, carry):
        count_ref[o] = 0
        return carry

    lax.fori_loop(0, owners, clear, 0, unroll=8)

    def move(t, carry):
        o = owner_ref[t]
        r = count_ref[o]
        count_ref[o] = r + 1
        place_ref[2 * o + r] = slot_ref[t]
        rows = patch_ref[pl.ds(pl.multiple_of(t * TILE, TILE), TILE), :]
        base = pl.multiple_of(r * 2 * TILE, TILE)
        out_ref[o, pl.ds(base, TILE), :] = rows[:, :128]
        out_ref[o, pl.ds(base + TILE, TILE), :] = rows[:, 128:]
        return carry

    lax.fori_loop(0, SLOTS, move, 0, unroll=8)
    row = lax.broadcasted_iota(jnp.int32, (PAY - 64, 128), 0)
    images = jnp.max(image_ref[...], axis=1, keepdims=True) + 1
    images = jnp.broadcast_to(images, row.shape)

    def label(o, carry):
        value = jnp.where(row == 0, place_ref[2 * o], jnp.where(row == 1, place_ref[2 * o + 1], images))
        out_ref[o, 64:, :] = value.astype(jnp.float32).astype(jnp.bfloat16)
        return carry

    lax.fori_loop(0, owners, label, 0, unroll=8)

    @pl.when(core == 0)
    def _():
        for copy in even:
            copy.wait()

    @pl.when(core != 0)
    def _():
        for copy in odd:
            copy.wait()


def send_pack(owner, slot, place, image, patches, weights, senders):
    return pl.pallas_call(
        send_kernel,
        grid_spec=pltpu.PrefetchScalarGridSpec(
            num_scalar_prefetch=3,
            grid=(1,),
            in_specs=[
                pl.BlockSpec((1, SLOTS), lambda i, a, b, m: (0, 0)),
                pl.BlockSpec((SLOTS * TILE, PW), lambda i, a, b, m: (0, m[0])),
            ]
            + [pl.BlockSpec(memory_space=pl.ANY)] * 4,
            out_specs=[pl.BlockSpec((senders, PAY, 128), lambda i, a, b, m: (0, 0, 0))]
            + [pl.BlockSpec((D, PW), lambda i, a, b, m: (0, 0))] * 2,
            scratch_shapes=[
                pltpu.SMEM((senders,), jnp.int32),
                pltpu.SMEM((2 * senders,), jnp.int32),
                pltpu.SemaphoreType.DMA((1 + PARTS,)),
            ],
        ),
        out_shape=[jax.ShapeDtypeStruct((senders, PAY, 128), jnp.bfloat16)]
        + [jax.ShapeDtypeStruct((D, PW), jnp.bfloat16)] * 2,
        compiler_params=VMEM,
        name="send_pack",
    )(owner, slot, place, image, patches, *weights)


def arrive_kernel(mp_ref, in_ref, out0, out1, out2, out3, total_ref, sorted_ref, label_ref, slot_ref, sems):
    senders = in_ref.shape[0]
    row = lax.broadcasted_iota(jnp.int32, (8, 128), 0)
    lane = lax.broadcasted_iota(jnp.int32, (8, 128), 1)
    picked = jnp.zeros((8, 128), jnp.float32)
    total = jnp.zeros((8, 128), jnp.float32)
    for s in range(senders):
        marks = in_ref[s, 64:, :].astype(jnp.float32)
        picked = jnp.where((lane == 2 * s) | (lane == 2 * s + 1), marks, picked)
        total = total + marks
    odd = (lane & 1) == 1
    own = jnp.where(row == jnp.where(odd, 1, 0), picked, 0.0)
    label_ref[...] = jnp.broadcast_to(jnp.sum(own, axis=0, keepdims=True), (8, 128)).astype(jnp.int32)
    copy = pltpu.make_async_copy(label_ref, slot_ref, sems.at[4])
    copy.start()
    total_ref[...] = jnp.broadcast_to(jnp.sum(jnp.where(row == 2, total, 0.0), axis=0, keepdims=True), (8, 128))
    sorted_ref[SLOTS * TILE :, :] = jnp.zeros((ROWS_W - PART_SLOTS * TILE, PW), jnp.bfloat16)
    copy.wait()

    def move(s, carry):
        for r in range(2):
            at = pl.multiple_of(slot_ref[0, 2 * s + r] * TILE, TILE)
            sorted_ref[pl.ds(at, TILE), :128] = in_ref[s, 2 * r * TILE : (2 * r + 1) * TILE, :]
            sorted_ref[pl.ds(at, TILE), 128:] = in_ref[s, (2 * r + 1) * TILE : (2 * r + 2) * TILE, :]
        return carry

    lax.fori_loop(0, senders, move, 0, unroll=8)
    copies = []
    for d, out in enumerate((out0, out1, out2, out3)):
        part = (mp_ref[0] + d) % PARTS
        at = pl.multiple_of(part * PART_SLOTS * TILE, TILE)
        copies.append(pltpu.make_async_copy(sorted_ref.at[pl.ds(at, ROWS_W), :], out, sems.at[d]))
    for copy in copies:
        copy.start()
    for copy in copies:
        copy.wait()


def arrive_sort(mp, incoming):
    window = jax.ShapeDtypeStruct((ROWS_W, PW), jnp.bfloat16)
    return pl.pallas_call(
        arrive_kernel,
        grid_spec=pltpu.PrefetchScalarGridSpec(
            num_scalar_prefetch=1,
            grid=(1,),
            in_specs=[pl.BlockSpec(incoming.shape, lambda i, a: (0, 0, 0))],
            out_specs=[pl.BlockSpec(memory_space=pl.ANY)] * PARTS + [pl.BlockSpec((8, 128), lambda i, a: (0, 0))],
            scratch_shapes=[
                pltpu.VMEM((SLOTS * TILE + ROWS_W - PART_SLOTS * TILE, PW), jnp.bfloat16),
                pltpu.VMEM((8, 128), jnp.int32),
                pltpu.SMEM((8, 128), jnp.int32),
                pltpu.SemaphoreType.DMA((5,)),
            ],
        ),
        out_shape=[window] * PARTS + [jax.ShapeDtypeStruct((8, 128), jnp.float32)],
        compiler_params=VMEM,
        name="arrive_sort",
    )(mp, incoming)


def block_kernel(place_ref, image_ref, x0, x1, x2, x3, wq, wk, wv, wo, a0, a1, a0x, a1x, b0, b1, b0x, b1x, c0, c1, c0x, c1x,
                 out0, out1, out2, out3, sum0, sum1, sum2, sum3,
                 x_ref, norm_ref, q_ref, k_ref, v_ref, att_ref, w_refs, begin_ref, end_ref, xsem, wsem):
    part = place_ref[0]
    core = place_ref[1]
    x_copies = []
    for d, x in enumerate((x0, x1, x2, x3)):
        x_copies.append(pltpu.make_async_copy(x, x_ref.at[(part + PARTS - d) % PARTS], xsem.at[d]))
        x_copies[-1].start()
    copies = [[pltpu.make_async_copy(w, w_refs.at[0, n], wsem.at[n]) for n, w in enumerate((wq, wk, wv))]]
    for n in range(PARTS):
        block_rows = pl.ds(n * PW, PW)
        copies[0].append(pltpu.make_async_copy(wo.at[:, block_rows], w_refs.at[0, 3, block_rows, :], wsem.at[4 * PARTS - 1 + n]))
    for g, (m0, m1, o0, o1) in enumerate(((a0, a1, a0x, a1x), (b0, b1, b0x, b1x), (c0, c1, c0x, c1x))):
        group = []
        for n, (w, place) in enumerate(((m0, 2 * core), (m1, 2 * core + 1), (o0, 2 - 2 * core), (o1, 3 - 2 * core))):
            group.append(pltpu.make_async_copy(w, w_refs.at[g + 1, place], wsem.at[4 * g + 3 + n]))
        copies.append(group)
    for group in copies:
        for copy in group:
            copy.start()

    window = part * PART_SLOTS
    for i in range(8):
        begin_ref[i] = 0
        end_ref[i] = 0

    def scan(l, carry):
        before, count, first, mine = carry
        t = window + l
        label = jnp.where(t < SLOTS, image_ref[jnp.minimum(t, SLOTS - 1)], -1)
        fresh = (label >= 0) & (label != before)
        starts = fresh & (l < PART_SLOTS)
        mine = jnp.where(fresh, jnp.where(starts, 1, 0), jnp.where(label >= 0, mine, 0))
        first = jnp.where(starts & (count == 0), label, first)
        count = count + jnp.where(starts, 1, 0)
        begin_ref[jnp.where(starts, count - 1, 7)] = l
        end_ref[jnp.where(mine == 1, count - 1, 7)] = l + 1
        return label, count, first, mine

    before = jnp.where(part > 0, image_ref[jnp.maximum(window - 1, 0)], -1)
    _, count, first, _ = lax.fori_loop(0, WIN, scan, (before, jnp.int32(0), jnp.int32(0), jnp.int32(0)), unroll=4)
    for copy in x_copies:
        copy.wait()

    chunk = 128

    def norm(i, carry):
        at = pl.multiple_of(i * chunk, chunk)
        rows = [x_ref[p, pl.ds(at, chunk), :].astype(jnp.float32) for p in range(PARTS)]
        mean = jnp.sum(rows[0] + rows[1] + rows[2] + rows[3], axis=-1, keepdims=True) * (1.0 / D)
        centred = [r - mean for r in rows]
        squares = [r * r for r in centred]
        spread = jnp.sum(squares[0] + squares[1] + squares[2] + squares[3], axis=-1, keepdims=True) * (1.0 / D)
        scale = lax.rsqrt(spread + EPSILON)
        for p in range(PARTS):
            norm_ref[pl.ds(at, chunk), p * PW : (p + 1) * PW] = (centred[p] * scale).astype(jnp.bfloat16)
        return carry

    lax.fori_loop(0, ROWS_W // chunk, norm, 0)
    lane = lax.broadcasted_iota(jnp.int32, (IMG_ROWS, PW), 1)
    upper = lax.broadcasted_iota(jnp.int32, (IMG_ROWS, 128), 1) + 128
    low = lax.broadcasted_iota(jnp.int32, (IMG_ROWS, 128), 1) < HD

    for g in range(PARTS):
        for copy in copies[g]:
            copy.wait()
        for n, ref in enumerate((q_ref, k_ref, v_ref)):
            ref[...] = jnp.dot(norm_ref[...], w_refs[g, n], preferred_element_type=jnp.float32).astype(jnp.bfloat16)

        def image(i, carry):
            row = pl.multiple_of(begin_ref[i] * TILE, TILE)
            limit = (end_ref[i] - begin_ref[i]) * TILE

            def mix(size):
                window = pl.ds(row, size)
                queries = q_ref[window, :]
                keys = k_ref[window, :]
                values = v_ref[window, :]
                allowed = lax.broadcasted_iota(jnp.int32, (size, size - 128), 1) + 128 < limit
                lane = lax.broadcasted_iota(jnp.int32, (size, PW), 1)
                low = lax.broadcasted_iota(jnp.int32, (size, 128), 1) < HD
                heads = range(PW // HD)
                inside = [(lane >= h * HD) & (lane < (h + 1) * HD) for h in heads]
                nears, fars = [], []
                scores = [
                    lax.dot_general(queries, jnp.where(inside[h], keys, jnp.zeros_like(keys)), (((1,), (1,)), ((), ())), preferred_element_type=jnp.float32)
                    for h in heads
                ]
                raised = []
                for h in heads:
                    always, maybe = scores[h][:, :128], jnp.where(allowed, scores[h][:, 128:], -1e30)
                    peak = jnp.maximum(jnp.max(always, axis=-1, keepdims=True), jnp.max(maybe, axis=-1, keepdims=True))
                    raised.append(jnp.exp2((jnp.concatenate([always, maybe], axis=1) - peak) * EXP_SCALE).astype(jnp.bfloat16))
                for h in heads:
                    mixed = jnp.dot(raised[h], jnp.where(inside[h], values, jnp.ones_like(values)), preferred_element_type=jnp.float32)
                    near, far = (mixed[:, :128], mixed[:, 128:]) if h < 2 else (mixed[:, 128:], mixed[:, :128])
                    nears.append(near)
                    fars.append(far)
                for half in range(2):
                    top = jnp.where(low, nears[2 * half], nears[2 * half + 1])
                    bottom = jnp.where(low, fars[2 * half], fars[2 * half + 1])
                    att_ref[window, g * PW + half * 128 : g * PW + (half + 1) * 128] = (top / bottom).astype(jnp.bfloat16)

            @pl.when(limit <= 192)
            def _():
                mix(192)

            @pl.when(limit > 192)
            def _():
                mix(256)

            return carry

        lax.fori_loop(0, count, image, 0)

    start_row = begin_ref[0] * TILE
    end_row = end_ref[0]
    for i in range(1, MAX_LOCAL):
        end_row = jnp.maximum(end_row, end_ref[i])
    end_row = end_row * TILE
    row_ids = lax.broadcasted_iota(jnp.int32, (ROWS_W, PW), 0)
    live = (row_ids >= start_row) & (row_ids < end_row)
    tile_ids = lax.broadcasted_iota(jnp.int32, (WIN, 8, PW), 0)
    pooled_ids = lax.broadcasted_iota(jnp.int32, (IMG, PW), 0)
    lengths = jnp.ones((IMG, PW), jnp.float32)
    tiles = []
    for i in range(MAX_LOCAL):
        tiles.append((tile_ids >= begin_ref[i]) & (tile_ids < end_ref[i]))
        rows_i = ((end_ref[i] - begin_ref[i]) * TILE).astype(jnp.float32)
        lengths = jnp.where((pooled_ids == first + i) & (rows_i > 0), rows_i, lengths)
    for d, (out, sum_ref) in enumerate(((out0, sum0), (out1, sum1), (out2, sum2), (out3, sum3))):
        n = (part + d) % PARTS
        block_rows = pl.ds(pl.multiple_of(n * PW, PW), PW)
        mix = jnp.concatenate([w_refs[g, 3, block_rows, :] for g in range(PARTS)], axis=0)
        projected = jnp.dot(att_ref[...], mix, preferred_element_type=jnp.float32)
        result = jnp.where(live, x_ref[n].astype(jnp.float32) + projected, 0.0)
        out[:ROWS_W, :] = result.astype(jnp.bfloat16)
        pairs = result.reshape(WIN, 2, 8, PW)
        pairs = pairs[:, 0] + pairs[:, 1]
        sums = jnp.zeros((IMG, PW), jnp.float32)
        for i in range(MAX_LOCAL):
            held = jnp.sum(jnp.where(tiles[i], pairs, 0.0), axis=0)
            sums = jnp.where(pooled_ids == first + i, jnp.sum(held, axis=0, keepdims=True), sums)
        pooled = sums / lengths
        one = pooled.astype(jnp.bfloat16)
        rest = pooled - one.astype(jnp.float32)
        two = rest.astype(jnp.bfloat16)
        three = (rest - two.astype(jnp.float32)).astype(jnp.bfloat16)
        out[ROWS_W : ROWS_W + IMG, :] = one
        out[ROWS_W + IMG : ROWS_W + 2 * IMG, :] = two
        out[ROWS_W + 2 * IMG : ROWS_W + 3 * IMG, :] = three
        sum_ref[...] = jnp.sum(pooled, axis=0, keepdims=True)


def block(place, image, xs, weights):
    outs = jax.ShapeDtypeStruct((ROWS_W + EXTRA, PW), jnp.bfloat16)
    whole = lambda i, a, b: (0, 0)
    wide = pltpu.VMEM((ROWS_W, PW), jnp.bfloat16)
    return pl.pallas_call(
        block_kernel,
        grid_spec=pltpu.PrefetchScalarGridSpec(
            num_scalar_prefetch=2,
            grid=(1,),
            in_specs=[pl.BlockSpec(memory_space=pl.ANY)] * (len(xs) + len(weights)),
            out_specs=[pl.BlockSpec((ROWS_W + EXTRA, PW), whole)] * PARTS + [pl.BlockSpec((1, PW), whole)] * PARTS,
            scratch_shapes=[
                pltpu.VMEM((PARTS, ROWS_W, PW), jnp.bfloat16),
                pltpu.VMEM((ROWS_W, D), jnp.bfloat16),
                wide,
                wide,
                wide,
                pltpu.VMEM((ROWS_W, D), jnp.bfloat16),
                pltpu.VMEM((PARTS, 4, D, PW), jnp.bfloat16),
                pltpu.SMEM((8,), jnp.int32),
                pltpu.SMEM((8,), jnp.int32),
                pltpu.SemaphoreType.DMA((PARTS,)),
                pltpu.SemaphoreType.DMA((5 * PARTS - 1,)),
            ],
        ),
        out_shape=[outs] * PARTS + [jax.ShapeDtypeStruct((1, PW), jnp.float32)] * PARTS,
        compiler_params=VMEM,
        name="block",
    )(place, image, *xs, *weights)


def finish_kernel(place_ref, r0, r1, r2, r3, out_ref, pooled_ref, in_ref, out_vmem, sems, out_sems):
    size = PART_SLOTS * TILE
    halo = ROWS_W - size
    part = place_ref[0]
    copies = []
    for d, r in enumerate((r0, r1, r2, r3)):
        copies.append(pltpu.make_async_copy(r, in_ref.at[(part + PARTS - d) % PARTS], sems.at[d]))
    for copy in copies:
        copy.start()
    for copy in copies:
        copy.wait()
    writes = []
    for p in range(PARTS):
        start = in_ref[p, :halo, :]
        if p:
            start = start + in_ref[p - 1, size:ROWS_W, :]
        out_vmem[p * size : p * size + halo, :] = start
        out_vmem[p * size + halo : (p + 1) * size, :] = in_ref[p, halo:size, :]
        rows = pl.ds(p * size, size)
        writes.append(pltpu.make_async_copy(out_vmem.at[rows, :], out_ref.at[rows, :], out_sems.at[p]))
        writes[-1].start()
    pooled = jnp.zeros((IMG, PW), jnp.float32)
    for p in range(PARTS):
        for n in range(3):
            pooled = pooled + in_ref[p, ROWS_W + n * IMG : ROWS_W + (n + 1) * IMG, :].astype(jnp.float32)
    pooled_ref[...] = pooled
    for write in writes:
        write.wait()


def finish(place, received):
    return pl.pallas_call(
        finish_kernel,
        grid_spec=pltpu.PrefetchScalarGridSpec(
            num_scalar_prefetch=1,
            grid=(1,),
            in_specs=[pl.BlockSpec(memory_space=pl.ANY)] * PARTS,
            out_specs=[pl.BlockSpec(memory_space=pl.ANY), pl.BlockSpec((IMG, PW), lambda i, a: (0, 0))],
            scratch_shapes=[
                pltpu.VMEM((PARTS, ROWS_W + EXTRA, PW), jnp.bfloat16),
                pltpu.VMEM((SLOTS * TILE, PW), jnp.bfloat16),
                pltpu.SemaphoreType.DMA((PARTS,)),
                pltpu.SemaphoreType.DMA((PARTS,)),
            ],
        ),
        out_shape=[
            jax.ShapeDtypeStruct((SLOTS * TILE, PW), jnp.bfloat16),
            jax.ShapeDtypeStruct((IMG, PW), jnp.float32),
        ],
        compiler_params=VMEM,
        name="finish",
    )(place, *received)


def pool_kernel(sums_ref, number_ref, pooled_ref, image_ref, out_ref):
    total = jnp.sum(sums_ref[...], axis=0)
    centre = jnp.concatenate([total[0:1], total[1:2]], axis=1) / number_ref[0:1, 0:1]
    slots = lax.broadcasted_iota(jnp.int32, (IMG, SLOTS), 0) == image_ref[...]
    present = jnp.max(jnp.where(slots, 1.0, 0.0), axis=1, keepdims=True) > 0.5
    out_ref[...] = jnp.where(present, pooled_ref[...] - centre, 0.0).astype(jnp.bfloat16)


def pool(sums, number, pooled, image):
    return pl.pallas_call(
        pool_kernel,
        out_shape=jax.ShapeDtypeStruct((IMG, PW), jnp.bfloat16),
        name="pool",
    )(sums, number, pooled, image)


def passed_on(pieces, shift):
    got = []
    for d in (1, 2, 3):
        got.append(lax.ppermute(pieces[d], "mp", shift(d)))
    return got


def whole_block(patches, dest_owner, dest_slot, packed_image, w_query, w_key, w_value, w_out):
    senders = lax.axis_size("dp")
    splits = lax.axis_size("mp")
    mp = lax.axis_index("mp").astype(jnp.int32)
    core = (lax.axis_index("dp") % 2).astype(jnp.int32)
    place = jnp.stack([mp, core])
    shift = lambda d: [(i, (i + d) % splits) for i in range(splits)]
    swap = [(i, i ^ 1) for i in range(senders)]

    own = (w_query, w_key, w_value, w_out)
    image = packed_image.reshape(1, SLOTS)
    outgoing, s0, s1 = send_pack(dest_owner, dest_slot, place, image, patches, own, senders)
    a0, a1 = (lax.ppermute(s, "mp", shift(1)) for s in (s0, s1))
    b0, b1 = (lax.ppermute(s, "mp", shift(-1)) for s in (s0, s1))
    c0 = lax.ppermute(a0, "mp", shift(1))
    c1 = lax.ppermute(b1, "mp", shift(-1))
    a0x, a1x, b0x, b1x, c0x, c1x = (lax.ppermute(w, "dp", swap) for w in (a0, a1, b0, b1, c0, c1))
    weights = own + (a0, a1, a0x, a1x, b0, b1, b0x, b1x, c0, c1, c0x, c1x)

    incoming = lax.all_to_all(outgoing, "dp", split_axis=0, concat_axis=0, tiled=True)
    *windows, number = arrive_sort(place[:1], incoming)
    rows = [windows[0]] + passed_on(windows, shift)
    outcome = block(place, packed_image, rows, weights)
    results, sums = outcome[:PARTS], outcome[PARTS:]
    total = sums[0] + sum(lax.ppermute(sums[d], "mp", shift(d)) for d in (1, 2, 3))
    received = [results[0]] + passed_on(results, shift)
    spread = jnp.broadcast_to(total.reshape(1, 2, PW // 2), (senders, 2, PW // 2))
    gathered = lax.all_to_all(spread, "dp", split_axis=0, concat_axis=0, tiled=True)
    packed_out, pooled = finish(place[:1], received)
    pooled_out = pool(gathered, number, pooled, image)
    return (packed_out, pooled_out)


def solution(mesh):
    in_specs = (
        P("dp", None),
        P("dp"),
        P("dp"),
        P("dp"),
        P(None, "mp"),
        P(None, "mp"),
        P(None, "mp"),
        P("mp", None),
    )
    out_specs = (P("dp", "mp"), P("dp", "mp"))
    return jax.shard_map(whole_block, mesh=mesh, in_specs=in_specs, out_specs=out_specs, check_vma=False)
```

```python
import jax
import jax.numpy as jnp
from jax import lax
from jax.experimental import pallas as pl
from jax.experimental.pallas import tpu as pltpu
from jax.sharding import PartitionSpec as P

EPSILON = 1e-06
SLOTS = 128
TILE = 16
D = 1024
PARTS = 4
PW = D // PARTS
PART_SLOTS = SLOTS // PARTS
WIN = PART_SLOTS + 15
ROWS_W = WIN * TILE
IMG = 16
EXTRA = 3 * IMG
HD = 64
MAX_LOCAL = 4
PAY = 72
EXP_SCALE = HD ** (-0.5) * 1.4426950408889634
VMEM = pltpu.CompilerParams(vmem_limit_bytes=56 * 1024 * 1024)


def send_kernel(owner_ref, slot_ref, mp_ref, core_ref, image_ref, patch_ref, wq, wk, wv, wo, out_ref, s0, s1, count_ref, place_ref, sems):
    owners = out_ref.shape[0]
    core = core_ref[0]
    even = [pltpu.make_async_copy(wq, s0, sems.at[0]), pltpu.make_async_copy(wk, s1, sems.at[1])]
    odd = [pltpu.make_async_copy(wv, s0, sems.at[0])]
    for n in range(PARTS):
        block_rows = pl.ds(n * PW, PW)
        odd.append(pltpu.make_async_copy(wo.at[:, block_rows], s1.at[block_rows, :], sems.at[1 + n]))

    @pl.when(core == 0)
    def _():
        for copy in even:
            copy.start()

    @pl.when(core != 0)
    def _():
        for copy in odd:
            copy.start()

    def clear(o, carry):
        count_ref[o] = 0
        return carry

    lax.fori_loop(0, owners, clear, 0, unroll=8)

    def move(t, carry):
        o = owner_ref[t]
        r = count_ref[o]
        count_ref[o] = r + 1
        place_ref[2 * o + r] = slot_ref[t]
        rows = patch_ref[pl.ds(pl.multiple_of(t * TILE, TILE), TILE), :]
        base = pl.multiple_of(r * 2 * TILE, TILE)
        out_ref[o, pl.ds(base, TILE), :] = rows[:, :128]
        out_ref[o, pl.ds(base + TILE, TILE), :] = rows[:, 128:]
        return carry

    lax.fori_loop(0, SLOTS, move, 0, unroll=8)
    row = lax.broadcasted_iota(jnp.int32, (PAY - 64, 128), 0)
    images = jnp.max(image_ref[...], axis=1, keepdims=True) + 1
    images = jnp.broadcast_to(images, row.shape)

    def label(o, carry):
        value = jnp.where(row == 0, place_ref[2 * o], jnp.where(row == 1, place_ref[2 * o + 1], images))
        out_ref[o, 64:, :] = value.astype(jnp.float32).astype(jnp.bfloat16)
        return carry

    lax.fori_loop(0, owners, label, 0, unroll=8)

    @pl.when(core == 0)
    def _():
        for copy in even:
            copy.wait()

    @pl.when(core != 0)
    def _():
        for copy in odd:
            copy.wait()


def send_pack(owner, slot, part, core, image, patches, weights, senders):
    return pl.pallas_call(
        send_kernel,
        grid_spec=pltpu.PrefetchScalarGridSpec(
            num_scalar_prefetch=4,
            grid=(1,),
            in_specs=[
                pl.BlockSpec((1, SLOTS), lambda i, a, b, m, c: (0, 0)),
                pl.BlockSpec((SLOTS * TILE, PW), lambda i, a, b, m, c: (0, m[0])),
            ]
            + [pl.BlockSpec(memory_space=pl.ANY)] * 4,
            out_specs=[pl.BlockSpec((senders, PAY, 128), lambda i, a, b, m, c: (0, 0, 0))]
            + [pl.BlockSpec((D, PW), lambda i, a, b, m, c: (0, 0))] * 2,
            scratch_shapes=[
                pltpu.SMEM((senders,), jnp.int32),
                pltpu.SMEM((2 * senders,), jnp.int32),
                pltpu.SemaphoreType.DMA((1 + PARTS,)),
            ],
        ),
        out_shape=[jax.ShapeDtypeStruct((senders, PAY, 128), jnp.bfloat16)]
        + [jax.ShapeDtypeStruct((D, PW), jnp.bfloat16)] * 2,
        compiler_params=VMEM,
        name="send_pack",
    )(owner, slot, part, core, image, patches, *weights)


def arrive_kernel(mp_ref, in_ref, out0, out1, out2, out3, total_ref, sorted_ref, label_ref, slot_ref, sems):
    senders = in_ref.shape[0]
    row = lax.broadcasted_iota(jnp.int32, (8, 128), 0)
    lane = lax.broadcasted_iota(jnp.int32, (8, 128), 1)
    picked = jnp.zeros((8, 128), jnp.float32)
    total = jnp.zeros((8, 128), jnp.float32)
    for s in range(senders):
        marks = in_ref[s, 64:, :].astype(jnp.float32)
        picked = jnp.where((lane == 2 * s) | (lane == 2 * s + 1), marks, picked)
        total = total + marks
    odd = (lane & 1) == 1
    own = jnp.where(row == jnp.where(odd, 1, 0), picked, 0.0)
    label_ref[...] = jnp.broadcast_to(jnp.sum(own, axis=0, keepdims=True), (8, 128)).astype(jnp.int32)
    copy = pltpu.make_async_copy(label_ref, slot_ref, sems.at[4])
    copy.start()
    total_ref[...] = jnp.broadcast_to(jnp.sum(jnp.where(row == 2, total, 0.0), axis=0, keepdims=True), (8, 128))
    sorted_ref[SLOTS * TILE :, :] = jnp.zeros((ROWS_W - PART_SLOTS * TILE, PW), jnp.bfloat16)
    copy.wait()

    def move(s, carry):
        for r in range(2):
            at = pl.multiple_of(slot_ref[0, 2 * s + r] * TILE, TILE)
            sorted_ref[pl.ds(at, TILE), :128] = in_ref[s, 2 * r * TILE : (2 * r + 1) * TILE, :]
            sorted_ref[pl.ds(at, TILE), 128:] = in_ref[s, (2 * r + 1) * TILE : (2 * r + 2) * TILE, :]
        return carry

    lax.fori_loop(0, senders, move, 0, unroll=8)
    copies = []
    for d, out in enumerate((out0, out1, out2, out3)):
        part = (mp_ref[0] + d) % PARTS
        at = pl.multiple_of(part * PART_SLOTS * TILE, TILE)
        copies.append(pltpu.make_async_copy(sorted_ref.at[pl.ds(at, ROWS_W), :], out, sems.at[d]))
    for copy in copies:
        copy.start()
    for copy in copies:
        copy.wait()


def arrive_sort(mp, incoming):
    window = jax.ShapeDtypeStruct((ROWS_W, PW), jnp.bfloat16)
    return pl.pallas_call(
        arrive_kernel,
        grid_spec=pltpu.PrefetchScalarGridSpec(
            num_scalar_prefetch=1,
            grid=(1,),
            in_specs=[pl.BlockSpec(memory_space=pltpu.VMEM)],
            out_specs=[pl.BlockSpec(memory_space=pl.ANY)] * PARTS + [pl.BlockSpec((8, 128), lambda i, a: (0, 0))],
            scratch_shapes=[
                pltpu.VMEM((SLOTS * TILE + ROWS_W - PART_SLOTS * TILE, PW), jnp.bfloat16),
                pltpu.VMEM((8, 128), jnp.int32),
                pltpu.SMEM((8, 128), jnp.int32),
                pltpu.SemaphoreType.DMA((5,)),
            ],
        ),
        out_shape=[window] * PARTS + [jax.ShapeDtypeStruct((8, 128), jnp.float32)],
        compiler_params=VMEM,
        name="arrive_sort",
    )(mp, incoming)


def block_kernel(part_ref, core_ref, image_ref, x0, x1, x2, x3, wq, wk, wv, wo, a0, a1, a0x, a1x, b0, b1, b0x, b1x, c0, c1, c0x, c1x,
                 out0, out1, out2, out3, sum0, sum1, sum2, sum3,
                 norm_ref, q_ref, k_ref, v_ref, att_ref, w_refs, begin_ref, end_ref, wsem):
    part = part_ref[0]
    core = core_ref[0]
    xs = (x0, x1, x2, x3)
    copies = [[pltpu.make_async_copy(w, w_refs.at[0, n], wsem.at[n]) for n, w in enumerate((wq, wk, wv))]]
    for n in range(PARTS):
        block_rows = pl.ds(n * PW, PW)
        copies[0].append(pltpu.make_async_copy(wo.at[:, block_rows], w_refs.at[0, 3, block_rows, :], wsem.at[4 * PARTS - 1 + n]))
    for g, (m0, m1, o0, o1) in enumerate(((a0, a1, a0x, a1x), (b0, b1, b0x, b1x), (c0, c1, c0x, c1x))):
        group = []
        for n, (w, place) in enumerate(((m0, 2 * core), (m1, 2 * core + 1), (o0, 2 - 2 * core), (o1, 3 - 2 * core))):
            group.append(pltpu.make_async_copy(w, w_refs.at[g + 1, place], wsem.at[4 * g + 3 + n]))
        copies.append(group)
    for group in copies:
        for copy in group:
            copy.start()

    window = part * PART_SLOTS
    for i in range(8):
        begin_ref[i] = 0
        end_ref[i] = 0

    def scan(l, carry):
        before, count, first, mine = carry
        t = window + l
        label = jnp.where(t < SLOTS, image_ref[jnp.minimum(t, SLOTS - 1)], -1)
        fresh = (label >= 0) & (label != before)
        starts = fresh & (l < PART_SLOTS)
        mine = jnp.where(fresh, jnp.where(starts, 1, 0), jnp.where(label >= 0, mine, 0))
        first = jnp.where(starts & (count == 0), label, first)
        count = count + jnp.where(starts, 1, 0)
        begin_ref[jnp.where(starts, count - 1, 7)] = l
        end_ref[jnp.where(mine == 1, count - 1, 7)] = l + 1
        return label, count, first, mine

    before = jnp.where(part > 0, image_ref[jnp.maximum(window - 1, 0)], -1)
    _, count, first, _ = lax.fori_loop(0, WIN + 1, scan, (before, jnp.int32(0), jnp.int32(0), jnp.int32(0)), unroll=4)

    chunk = 128

    def norm(i, carry):
        at = pl.multiple_of(jnp.minimum(i * chunk, ROWS_W - chunk), TILE)
        rows = [x[pl.ds(at, chunk), :].astype(jnp.float32) for x in xs]
        mean = jnp.sum(rows[0] + rows[1] + rows[2] + rows[3], axis=-1, keepdims=True) * (1.0 / D)
        centred = [r - mean for r in rows]
        squares = [r * r for r in centred]
        spread = jnp.sum(squares[0] + squares[1] + squares[2] + squares[3], axis=-1, keepdims=True) * (1.0 / D)
        scale = lax.rsqrt(spread + EPSILON)
        for d in range(PARTS):
            norm_ref[(part + PARTS - d) % PARTS, pl.ds(at, chunk), :] = (centred[d] * scale).astype(jnp.bfloat16)
        return carry

    lax.fori_loop(0, pl.cdiv(ROWS_W, chunk), norm, 0)

    for g in range(PARTS):
        for copy in copies[g]:
            copy.wait()
        for n, ref in enumerate((q_ref, k_ref, v_ref)):
            normed = jnp.concatenate([norm_ref[p] for p in range(PARTS)], axis=1)
            ref[...] = jnp.dot(normed, w_refs[g, n], preferred_element_type=jnp.float32).astype(jnp.bfloat16)

        def image(i, carry):
            row = pl.multiple_of(begin_ref[i] * TILE, TILE)
            limit = (end_ref[i] - begin_ref[i]) * TILE

            def mix(size):
                window = pl.ds(row, size)
                queries = q_ref[window, :]
                keys = k_ref[window, :]
                values = v_ref[window, :]
                allowed = lax.broadcasted_iota(jnp.int32, (size, size - 128), 1) + 128 < limit
                lane = lax.broadcasted_iota(jnp.int32, (size, PW), 1)
                low = lax.broadcasted_iota(jnp.int32, (size, 128), 1) < HD
                heads = range(PW // HD)
                inside = [(lane >= h * HD) & (lane < (h + 1) * HD) for h in heads]
                nears, fars = [], []
                scores = [
                    lax.dot_general(queries, jnp.where(inside[h], keys, jnp.zeros_like(keys)), (((1,), (1,)), ((), ())), preferred_element_type=jnp.float32)
                    for h in heads
                ]
                raised = []
                for h in heads:
                    always, maybe = scores[h][:, :128], jnp.where(allowed, scores[h][:, 128:], -1e30)
                    peak = jnp.maximum(jnp.max(always, axis=-1, keepdims=True), jnp.max(maybe, axis=-1, keepdims=True))
                    raised.append(jnp.exp2((jnp.concatenate([always, maybe], axis=1) - peak) * EXP_SCALE).astype(jnp.bfloat16))
                for h in heads:
                    mixed = jnp.dot(raised[h], jnp.where(inside[h], values, jnp.ones_like(values)), preferred_element_type=jnp.float32)
                    near, far = (mixed[:, :128], mixed[:, 128:]) if h < 2 else (mixed[:, 128:], mixed[:, :128])
                    nears.append(near)
                    fars.append(far)
                for half in range(2):
                    top = jnp.where(low, nears[2 * half], nears[2 * half + 1])
                    bottom = jnp.where(low, fars[2 * half], fars[2 * half + 1])
                    att_ref[window, g * PW + half * 128 : g * PW + (half + 1) * 128] = (top / bottom).astype(jnp.bfloat16)

            @pl.when(limit <= 192)
            def _():
                mix(192)

            @pl.when(limit > 192)
            def _():
                mix(256)

            return carry

        lax.fori_loop(0, count, image, 0)

    start_row = begin_ref[0] * TILE
    end_row = end_ref[0]
    for i in range(1, MAX_LOCAL):
        end_row = jnp.maximum(end_row, end_ref[i])
    end_row = end_row * TILE
    row_ids = lax.broadcasted_iota(jnp.int32, (ROWS_W, PW), 0)
    live = (row_ids >= start_row) & (row_ids < end_row)
    tile_ids = lax.broadcasted_iota(jnp.int32, (WIN, 8, PW), 0)
    pooled_ids = lax.broadcasted_iota(jnp.int32, (IMG, PW), 0)
    lengths = jnp.ones((IMG, PW), jnp.float32)
    tiles = []
    for i in range(MAX_LOCAL):
        tiles.append((tile_ids >= begin_ref[i]) & (tile_ids < end_ref[i]))
        rows_i = ((end_ref[i] - begin_ref[i]) * TILE).astype(jnp.float32)
        lengths = jnp.where((pooled_ids == first + i) & (rows_i > 0), rows_i, lengths)
    for d, (out, sum_ref) in enumerate(((out0, sum0), (out1, sum1), (out2, sum2), (out3, sum3))):
        n = (part + d) % PARTS
        block_rows = pl.ds(pl.multiple_of(n * PW, PW), PW)
        mix = jnp.concatenate([w_refs[g, 3, block_rows, :] for g in range(PARTS)], axis=0)
        projected = jnp.dot(att_ref[...], mix, preferred_element_type=jnp.float32)
        result = jnp.where(live, xs[-d % PARTS][...].astype(jnp.float32) + projected, 0.0)
        out[:ROWS_W, :] = result.astype(jnp.bfloat16)
        pairs = result.reshape(WIN, 2, 8, PW)
        pairs = pairs[:, 0] + pairs[:, 1]
        sums = jnp.zeros((IMG, PW), jnp.float32)
        for i in range(MAX_LOCAL):
            held = jnp.sum(jnp.where(tiles[i], pairs, 0.0), axis=0)
            sums = jnp.where(pooled_ids == first + i, jnp.sum(held, axis=0, keepdims=True), sums)
        pooled = sums / lengths
        one = pooled.astype(jnp.bfloat16)
        rest = pooled - one.astype(jnp.float32)
        two = rest.astype(jnp.bfloat16)
        three = (rest - two.astype(jnp.float32)).astype(jnp.bfloat16)
        out[ROWS_W : ROWS_W + IMG, :] = one
        out[ROWS_W + IMG : ROWS_W + 2 * IMG, :] = two
        out[ROWS_W + 2 * IMG : ROWS_W + 3 * IMG, :] = three
        sum_ref[...] = jnp.sum(pooled, axis=0, keepdims=True)


def block(part, core, image, xs, weights):
    outs = jax.ShapeDtypeStruct((ROWS_W + EXTRA, PW), jnp.bfloat16)
    whole = lambda i, a, b, c: (0, 0)
    wide = pltpu.VMEM((ROWS_W, PW), jnp.bfloat16)
    return pl.pallas_call(
        block_kernel,
        grid_spec=pltpu.PrefetchScalarGridSpec(
            num_scalar_prefetch=3,
            grid=(1,),
            in_specs=[pl.BlockSpec(memory_space=pltpu.VMEM)] * len(xs)
            + [pl.BlockSpec(memory_space=pl.ANY)] * len(weights),
            out_specs=[pl.BlockSpec((ROWS_W + EXTRA, PW), whole)] * PARTS + [pl.BlockSpec((1, PW), whole)] * PARTS,
            scratch_shapes=[
                pltpu.VMEM((PARTS, ROWS_W, PW), jnp.bfloat16),
                wide,
                wide,
                wide,
                pltpu.VMEM((ROWS_W, D), jnp.bfloat16),
                pltpu.VMEM((PARTS, 4, D, PW), jnp.bfloat16),
                pltpu.SMEM((8,), jnp.int32),
                pltpu.SMEM((8,), jnp.int32),
                pltpu.SemaphoreType.DMA((5 * PARTS - 1,)),
            ],
        ),
        out_shape=[outs] * PARTS + [jax.ShapeDtypeStruct((1, PW), jnp.float32)] * PARTS,
        compiler_params=VMEM,
        name="block",
    )(part, core, image, *xs, *weights)


def finish_kernel(part_ref, r0, r1, r2, r3, out_ref, pooled_ref, out_vmem, sems):
    size = PART_SLOTS * TILE
    halo = ROWS_W - size
    received = (r0, r1, r2, r3)
    writes = []
    pooled = jnp.zeros((IMG, PW), jnp.float32)
    for d, r in enumerate(received):
        p = (part_ref[0] + PARTS - d) % PARTS
        base = pl.multiple_of(p * size, size)
        before = received[(d + 1) % PARTS][size:ROWS_W, :]
        start = r[:halo, :] + jnp.where(p > 0, before, jnp.zeros_like(before))
        out_vmem[pl.ds(base, halo), :] = start
        out_vmem[pl.ds(pl.multiple_of(base + halo, TILE), size - halo), :] = r[halo:size, :]
        rows = pl.ds(base, size)
        writes.append(pltpu.make_async_copy(out_vmem.at[rows, :], out_ref.at[rows, :], sems.at[d]))
        writes[-1].start()
        for n in range(3):
            pooled = pooled + r[ROWS_W + n * IMG : ROWS_W + (n + 1) * IMG, :].astype(jnp.float32)
    pooled_ref[...] = pooled
    for write in writes:
        write.wait()


def finish(part, received):
    return pl.pallas_call(
        finish_kernel,
        grid_spec=pltpu.PrefetchScalarGridSpec(
            num_scalar_prefetch=1,
            grid=(1,),
            in_specs=[pl.BlockSpec(memory_space=pltpu.VMEM)] * PARTS,
            out_specs=[pl.BlockSpec(memory_space=pl.ANY), pl.BlockSpec((IMG, PW), lambda i, a: (0, 0))],
            scratch_shapes=[
                pltpu.VMEM((SLOTS * TILE, PW), jnp.bfloat16),
                pltpu.SemaphoreType.DMA((PARTS,)),
            ],
        ),
        out_shape=[
            jax.ShapeDtypeStruct((SLOTS * TILE, PW), jnp.bfloat16),
            jax.ShapeDtypeStruct((IMG, PW), jnp.float32),
        ],
        compiler_params=VMEM,
        name="finish",
    )(part, *received)


def pool_kernel(sums_ref, number_ref, pooled_ref, image_ref, out_ref):
    total = jnp.sum(sums_ref[...], axis=0)
    centre = jnp.concatenate([total[0:1], total[1:2]], axis=1) / number_ref[0:1, 0:1]
    slots = lax.broadcasted_iota(jnp.int32, (IMG, SLOTS), 0) == image_ref[...]
    present = jnp.max(jnp.where(slots, 1.0, 0.0), axis=1, keepdims=True) > 0.5
    out_ref[...] = jnp.where(present, pooled_ref[...] - centre, 0.0).astype(jnp.bfloat16)


def pool(sums, number, pooled, image):
    return pl.pallas_call(
        pool_kernel,
        in_specs=[pl.BlockSpec(memory_space=pltpu.VMEM)] * 4,
        out_shape=jax.ShapeDtypeStruct((IMG, PW), jnp.bfloat16),
        name="pool",
    )(sums, number, pooled, image)


def passed_on(pieces, shift):
    got = []
    for d in (1, 2, 3):
        got.append(lax.ppermute(pieces[d], "mp", shift(d)))
    return got


def whole_block(patches, dest_owner, dest_slot, packed_image, w_query, w_key, w_value, w_out):
    senders = lax.axis_size("dp")
    splits = lax.axis_size("mp")
    part = lax.axis_index("mp").astype(jnp.int32).reshape(1)
    core = (lax.axis_index("dp").astype(jnp.int32) & 1).reshape(1)
    near = lambda array: pltpu.with_memory_space_constraint(array, pltpu.VMEM)
    shift = lambda d: [(i, (i + d) % splits) for i in range(splits)]
    swap = [(i, i ^ 1) for i in range(senders)]

    own = (w_query, w_key, w_value, w_out)
    image = packed_image.reshape(1, SLOTS)
    outgoing, s0, s1 = send_pack(dest_owner, dest_slot, part, core, image, patches, own, senders)
    a0, a1 = (lax.ppermute(s, "mp", shift(1)) for s in (s0, s1))
    b0, b1 = (lax.ppermute(s, "mp", shift(-1)) for s in (s0, s1))
    c0 = lax.ppermute(a0, "mp", shift(1))
    c1 = lax.ppermute(b1, "mp", shift(-1))
    a0x, a1x, b0x, b1x, c0x, c1x = (lax.ppermute(w, "dp", swap) for w in (a0, a1, b0, b1, c0, c1))
    weights = own + (a0, a1, a0x, a1x, b0, b1, b0x, b1x, c0, c1, c0x, c1x)

    incoming = lax.all_to_all(outgoing, "dp", split_axis=0, concat_axis=0, tiled=True)
    *windows, number = arrive_sort(part, near(incoming))
    rows = [windows[0]] + passed_on(windows, shift)
    outcome = block(part, core, packed_image, [near(r) for r in rows], weights)
    results, sums = outcome[:PARTS], outcome[PARTS:]
    total = sums[0] + sum(lax.ppermute(sums[d], "mp", shift(d)) for d in (1, 2, 3))
    received = [results[0]] + passed_on(results, shift)
    spread = jnp.broadcast_to(total.reshape(1, 2, PW // 2), (senders, 2, PW // 2))
    gathered = lax.all_to_all(spread, "dp", split_axis=0, concat_axis=0, tiled=True)
    packed_out, pooled = finish(part, [near(r) for r in received])
    pooled_out = pool(near(gathered), number, pooled, image)
    return (packed_out, pooled_out)


def solution(mesh):
    in_specs = (
        P("dp", None),
        P("dp"),
        P("dp"),
        P("dp"),
        P(None, "mp"),
        P(None, "mp"),
        P(None, "mp"),
        P("mp", None),
    )
    out_specs = (P("dp", "mp"), P("dp", "mp"))
    return jax.shard_map(whole_block, mesh=mesh, in_specs=in_specs, out_specs=out_specs, check_vma=False)
```

```python
import jax
import jax.numpy as jnp
from jax import lax
from jax.experimental import pallas as pl
from jax.experimental.pallas import tpu as pltpu
from jax.sharding import PartitionSpec as P

EPSILON = 1e-06
SLOTS = 128
TILE = 16
D = 1024
PARTS = 4
PW = D // PARTS
PART_SLOTS = SLOTS // PARTS
WIN = PART_SLOTS + 15
ROWS_W = WIN * TILE
IMG = 16
EXTRA = 3 * IMG
HD = 64
MAX_LOCAL = 4
PAY = 72
EXP_SCALE = HD ** (-0.5) * 1.4426950408889634
VMEM = pltpu.CompilerParams(vmem_limit_bytes=56 * 1024 * 1024)
MIDDLE = pltpu.CompilerParams(vmem_limit_bytes=32 * 1024 * 1024)
SMALL = pltpu.CompilerParams(vmem_limit_bytes=16 * 1024 * 1024)


def send_kernel(owner_ref, slot_ref, mp_ref, core_ref, image_ref, patch_ref, wq, wk, wv, wo, out_ref, s0, s1, count_ref, place_ref, sems):
    owners = out_ref.shape[0]
    core = core_ref[0]
    even = [pltpu.make_async_copy(wq, s0, sems.at[0]), pltpu.make_async_copy(wk, s1, sems.at[1])]
    odd = [pltpu.make_async_copy(wv, s0, sems.at[0])]
    for n in range(PARTS):
        block_rows = pl.ds(n * PW, PW)
        odd.append(pltpu.make_async_copy(wo.at[:, block_rows], s1.at[block_rows, :], sems.at[1 + n]))

    @pl.when(core == 0)
    def _():
        for copy in even:
            copy.start()

    @pl.when(core != 0)
    def _():
        for copy in odd:
            copy.start()

    def clear(o, carry):
        count_ref[o] = 0
        return carry

    lax.fori_loop(0, owners, clear, 0, unroll=8)

    def move(t, carry):
        o = owner_ref[t]
        r = count_ref[o]
        count_ref[o] = r + 1
        place_ref[2 * o + r] = slot_ref[t]
        rows = patch_ref[pl.ds(pl.multiple_of(t * TILE, TILE), TILE), :]
        base = pl.multiple_of(r * 2 * TILE, TILE)
        out_ref[o, pl.ds(base, TILE), :] = rows[:, :128]
        out_ref[o, pl.ds(base + TILE, TILE), :] = rows[:, 128:]
        return carry

    lax.fori_loop(0, SLOTS, move, 0, unroll=8)
    row = lax.broadcasted_iota(jnp.int32, (PAY - 64, 128), 0)
    images = jnp.max(image_ref[...], axis=1, keepdims=True) + 1
    images = jnp.broadcast_to(images, row.shape)

    def label(o, carry):
        value = jnp.where(row == 0, place_ref[2 * o], jnp.where(row == 1, place_ref[2 * o + 1], images))
        out_ref[o, 64:, :] = value.astype(jnp.float32).astype(jnp.bfloat16)
        return carry

    lax.fori_loop(0, owners, label, 0, unroll=8)

    @pl.when(core == 0)
    def _():
        for copy in even:
            copy.wait()

    @pl.when(core != 0)
    def _():
        for copy in odd:
            copy.wait()


def send_pack(owner, slot, part, core, image, patches, weights, senders):
    return pl.pallas_call(
        send_kernel,
        grid_spec=pltpu.PrefetchScalarGridSpec(
            num_scalar_prefetch=4,
            grid=(1,),
            in_specs=[
                pl.BlockSpec((1, SLOTS), lambda i, a, b, m, c: (0, 0)),
                pl.BlockSpec((SLOTS * TILE, PW), lambda i, a, b, m, c: (0, m[0])),
            ]
            + [pl.BlockSpec(memory_space=pl.ANY)] * 4,
            out_specs=[pl.BlockSpec((senders, PAY, 128), lambda i, a, b, m, c: (0, 0, 0))]
            + [pl.BlockSpec((D, PW), lambda i, a, b, m, c: (0, 0))] * 2,
            scratch_shapes=[
                pltpu.SMEM((senders,), jnp.int32),
                pltpu.SMEM((2 * senders,), jnp.int32),
                pltpu.SemaphoreType.DMA((1 + PARTS,)),
            ],
        ),
        out_shape=[jax.ShapeDtypeStruct((senders, PAY, 128), jnp.bfloat16)]
        + [jax.ShapeDtypeStruct((D, PW), jnp.bfloat16)] * 2,
        compiler_params=VMEM,
        name="send_pack",
    )(owner, slot, part, core, image, patches, *weights)


def arrive_kernel(mp_ref, in_ref, out0, out1, out2, out3, total_ref, sorted_ref, label_ref, slot_ref, sem):
    senders = in_ref.shape[0]
    row = lax.broadcasted_iota(jnp.int32, (8, 128), 0)
    lane = lax.broadcasted_iota(jnp.int32, (8, 128), 1)
    picked = jnp.zeros((8, 128), jnp.float32)
    total = jnp.zeros((8, 128), jnp.float32)
    for s in range(senders):
        marks = in_ref[s, 64:, :].astype(jnp.float32)
        picked = jnp.where((lane == 2 * s) | (lane == 2 * s + 1), marks, picked)
        total = total + marks
    odd = (lane & 1) == 1
    own = jnp.where(row == jnp.where(odd, 1, 0), picked, 0.0)
    label_ref[...] = jnp.broadcast_to(jnp.sum(own, axis=0, keepdims=True), (8, 128)).astype(jnp.int32)
    copy = pltpu.make_async_copy(label_ref, slot_ref, sem)
    copy.start()
    total_ref[...] = jnp.broadcast_to(jnp.sum(jnp.where(row == 2, total, 0.0), axis=0, keepdims=True), (8, 128))
    sorted_ref[SLOTS * TILE :, :] = jnp.zeros((ROWS_W - PART_SLOTS * TILE, PW), jnp.bfloat16)
    copy.wait()

    def move(s, carry):
        for r in range(2):
            at = pl.multiple_of(slot_ref[0, 2 * s + r] * TILE, TILE)
            sorted_ref[pl.ds(at, TILE), :128] = in_ref[s, 2 * r * TILE : (2 * r + 1) * TILE, :]
            sorted_ref[pl.ds(at, TILE), 128:] = in_ref[s, (2 * r + 1) * TILE : (2 * r + 2) * TILE, :]
        return carry

    lax.fori_loop(0, senders, move, 0, unroll=8)
    for d, out in enumerate((out0, out1, out2, out3)):
        part = (mp_ref[0] + d) % PARTS
        at = pl.multiple_of(part * PART_SLOTS * TILE, TILE)
        out[...] = sorted_ref[pl.ds(at, ROWS_W), :]


def arrive_sort(mp, incoming):
    window = jax.ShapeDtypeStruct((ROWS_W, PW), jnp.bfloat16)
    return pl.pallas_call(
        arrive_kernel,
        grid_spec=pltpu.PrefetchScalarGridSpec(
            num_scalar_prefetch=1,
            grid=(1,),
            in_specs=[pl.BlockSpec(memory_space=pltpu.VMEM)],
            out_specs=[pl.BlockSpec(memory_space=pltpu.VMEM)] * (PARTS + 1),
            scratch_shapes=[
                pltpu.VMEM((SLOTS * TILE + ROWS_W - PART_SLOTS * TILE, PW), jnp.bfloat16),
                pltpu.VMEM((8, 128), jnp.int32),
                pltpu.SMEM((8, 128), jnp.int32),
                pltpu.SemaphoreType.DMA,
            ],
        ),
        out_shape=[window] * PARTS + [jax.ShapeDtypeStruct((8, 128), jnp.float32)],
        compiler_params=SMALL,
        name="arrive_sort",
    )(mp, incoming)


def block_kernel(part_ref, core_ref, image_ref, x0, x1, x2, x3, wq, wk, wv, wo, a0, a1, a0x, a1x, b0, b1, b0x, b1x, c0, c1, c0x, c1x,
                 out0, out1, out2, out3, sum0, sum1, sum2, sum3,
                 norm_ref, q_ref, k_ref, v_ref, att_ref, w_refs, begin_ref, end_ref, wsem):
    part = part_ref[0]
    core = core_ref[0]
    xs = (x0, x1, x2, x3)
    copies = [[pltpu.make_async_copy(w, w_refs.at[0, n], wsem.at[n]) for n, w in enumerate((wq, wk, wv))]]
    for n in range(PARTS):
        block_rows = pl.ds(n * PW, PW)
        copies[0].append(pltpu.make_async_copy(wo.at[:, block_rows], w_refs.at[0, 3, block_rows, :], wsem.at[4 * PARTS - 1 + n]))
    for g, (m0, m1, o0, o1) in enumerate(((a0, a1, a0x, a1x), (b0, b1, b0x, b1x), (c0, c1, c0x, c1x))):
        group = []
        for n, (w, place) in enumerate(((m0, 2 * core), (m1, 2 * core + 1), (o0, 2 - 2 * core), (o1, 3 - 2 * core))):
            group.append(pltpu.make_async_copy(w, w_refs.at[g + 1, place], wsem.at[4 * g + 3 + n]))
        copies.append(group)
    for group in copies:
        for copy in group:
            copy.start()

    window = part * PART_SLOTS
    for i in range(8):
        begin_ref[i] = 0
        end_ref[i] = 0

    def scan(l, carry):
        before, count, first, mine = carry
        t = window + l
        label = jnp.where(t < SLOTS, image_ref[jnp.minimum(t, SLOTS - 1)], -1)
        fresh = (label >= 0) & (label != before)
        starts = fresh & (l < PART_SLOTS)
        mine = jnp.where(fresh, jnp.where(starts, 1, 0), jnp.where(label >= 0, mine, 0))
        first = jnp.where(starts & (count == 0), label, first)
        count = count + jnp.where(starts, 1, 0)
        begin_ref[jnp.where(starts, count - 1, 7)] = l
        end_ref[jnp.where(mine == 1, count - 1, 7)] = l + 1
        return label, count, first, mine

    before = jnp.where(part > 0, image_ref[jnp.maximum(window - 1, 0)], -1)
    _, count, first, _ = lax.fori_loop(0, WIN + 1, scan, (before, jnp.int32(0), jnp.int32(0), jnp.int32(0)), unroll=4)

    chunk = 128

    def norm(i, carry):
        at = pl.multiple_of(jnp.minimum(i * chunk, ROWS_W - chunk), TILE)
        rows = [x[pl.ds(at, chunk), :].astype(jnp.float32) for x in xs]
        mean = jnp.sum(rows[0] + rows[1] + rows[2] + rows[3], axis=-1, keepdims=True) * (1.0 / D)
        centred = [r - mean for r in rows]
        squares = [r * r for r in centred]
        spread = jnp.sum(squares[0] + squares[1] + squares[2] + squares[3], axis=-1, keepdims=True) * (1.0 / D)
        scale = lax.rsqrt(spread + EPSILON)
        for d in range(PARTS):
            norm_ref[(part + PARTS - d) % PARTS, pl.ds(at, chunk), :] = (centred[d] * scale).astype(jnp.bfloat16)
        return carry

    lax.fori_loop(0, pl.cdiv(ROWS_W, chunk), norm, 0)

    for g in range(PARTS):
        for copy in copies[g]:
            copy.wait()
        for n, ref in enumerate((q_ref, k_ref, v_ref)):
            normed = jnp.concatenate([norm_ref[p] for p in range(PARTS)], axis=1)
            ref[...] = jnp.dot(normed, w_refs[g, n], preferred_element_type=jnp.float32).astype(jnp.bfloat16)

        def image(i, carry):
            row = pl.multiple_of(begin_ref[i] * TILE, TILE)
            limit = (end_ref[i] - begin_ref[i]) * TILE

            def mix(size):
                window = pl.ds(row, size)
                queries = q_ref[window, :]
                keys = k_ref[window, :]
                values = v_ref[window, :]
                allowed = lax.broadcasted_iota(jnp.int32, (size, size - 128), 1) + 128 < limit
                lane = lax.broadcasted_iota(jnp.int32, (size, PW), 1)
                low = lax.broadcasted_iota(jnp.int32, (size, 128), 1) < HD
                heads = range(PW // HD)
                inside = [(lane >= h * HD) & (lane < (h + 1) * HD) for h in heads]
                nears, fars = [], []
                scores = [
                    lax.dot_general(queries, jnp.where(inside[h], keys, jnp.zeros_like(keys)), (((1,), (1,)), ((), ())), preferred_element_type=jnp.float32)
                    for h in heads
                ]
                raised = []
                for h in heads:
                    always, maybe = scores[h][:, :128], jnp.where(allowed, scores[h][:, 128:], -1e30)
                    peak = jnp.maximum(jnp.max(always, axis=-1, keepdims=True), jnp.max(maybe, axis=-1, keepdims=True))
                    raised.append(jnp.exp2((jnp.concatenate([always, maybe], axis=1) - peak) * EXP_SCALE).astype(jnp.bfloat16))
                for h in heads:
                    mixed = jnp.dot(raised[h], jnp.where(inside[h], values, jnp.ones_like(values)), preferred_element_type=jnp.float32)
                    near, far = (mixed[:, :128], mixed[:, 128:]) if h < 2 else (mixed[:, 128:], mixed[:, :128])
                    nears.append(near)
                    fars.append(far)
                for half in range(2):
                    top = jnp.where(low, nears[2 * half], nears[2 * half + 1])
                    bottom = jnp.where(low, fars[2 * half], fars[2 * half + 1])
                    att_ref[window, g * PW + half * 128 : g * PW + (half + 1) * 128] = (top / bottom).astype(jnp.bfloat16)

            @pl.when(limit <= 192)
            def _():
                mix(192)

            @pl.when(limit > 192)
            def _():
                mix(256)

            return carry

        lax.fori_loop(0, count, image, 0)

    start_row = begin_ref[0] * TILE
    end_row = end_ref[0]
    for i in range(1, MAX_LOCAL):
        end_row = jnp.maximum(end_row, end_ref[i])
    end_row = end_row * TILE
    row_ids = lax.broadcasted_iota(jnp.int32, (ROWS_W, PW), 0)
    live = (row_ids >= start_row) & (row_ids < end_row)
    tile_ids = lax.broadcasted_iota(jnp.int32, (WIN, 8, PW), 0)
    pooled_ids = lax.broadcasted_iota(jnp.int32, (IMG, PW), 0)
    lengths = jnp.ones((IMG, PW), jnp.float32)
    tiles = []
    for i in range(MAX_LOCAL):
        tiles.append((tile_ids >= begin_ref[i]) & (tile_ids < end_ref[i]))
        rows_i = ((end_ref[i] - begin_ref[i]) * TILE).astype(jnp.float32)
        lengths = jnp.where((pooled_ids == first + i) & (rows_i > 0), rows_i, lengths)
    for d, (out, sum_ref) in enumerate(((out0, sum0), (out1, sum1), (out2, sum2), (out3, sum3))):
        n = (part + d) % PARTS
        block_rows = pl.ds(pl.multiple_of(n * PW, PW), PW)
        mix = jnp.concatenate([w_refs[g, 3, block_rows, :] for g in range(PARTS)], axis=0)
        projected = jnp.dot(att_ref[...], mix, preferred_element_type=jnp.float32)
        result = jnp.where(live, xs[-d % PARTS][...].astype(jnp.float32) + projected, 0.0)
        out[:ROWS_W, :] = result.astype(jnp.bfloat16)
        pairs = result.reshape(WIN, 2, 8, PW)
        pairs = pairs[:, 0] + pairs[:, 1]
        sums = jnp.zeros((IMG, PW), jnp.float32)
        for i in range(MAX_LOCAL):
            held = jnp.sum(jnp.where(tiles[i], pairs, 0.0), axis=0)
            sums = jnp.where(pooled_ids == first + i, jnp.sum(held, axis=0, keepdims=True), sums)
        pooled = sums / lengths
        one = pooled.astype(jnp.bfloat16)
        rest = pooled - one.astype(jnp.float32)
        two = rest.astype(jnp.bfloat16)
        three = (rest - two.astype(jnp.float32)).astype(jnp.bfloat16)
        out[ROWS_W : ROWS_W + IMG, :] = one
        out[ROWS_W + IMG : ROWS_W + 2 * IMG, :] = two
        out[ROWS_W + 2 * IMG : ROWS_W + 3 * IMG, :] = three
        line = jnp.sum(pooled, axis=0, keepdims=True)
        sum_ref[0:1, :] = line[:, : PW // 2]
        sum_ref[1:2, :] = line[:, PW // 2 :]


def block(part, core, image, xs, weights):
    outs = jax.ShapeDtypeStruct((ROWS_W + EXTRA, PW), jnp.bfloat16)
    wide = pltpu.VMEM((ROWS_W, PW), jnp.bfloat16)
    return pl.pallas_call(
        block_kernel,
        grid_spec=pltpu.PrefetchScalarGridSpec(
            num_scalar_prefetch=3,
            grid=(1,),
            in_specs=[pl.BlockSpec(memory_space=pltpu.VMEM)] * len(xs)
            + [pl.BlockSpec(memory_space=pltpu.HBM)] * len(weights),
            out_specs=[pl.BlockSpec(memory_space=pltpu.VMEM)] * (2 * PARTS),
            scratch_shapes=[
                pltpu.VMEM((PARTS, ROWS_W, PW), jnp.bfloat16),
                wide,
                wide,
                wide,
                pltpu.VMEM((ROWS_W, D), jnp.bfloat16),
                pltpu.VMEM((PARTS, 4, D, PW), jnp.bfloat16),
                pltpu.SMEM((8,), jnp.int32),
                pltpu.SMEM((8,), jnp.int32),
                pltpu.SemaphoreType.DMA((5 * PARTS - 1,)),
            ],
        ),
        out_shape=[outs] * PARTS + [jax.ShapeDtypeStruct((2, PW // 2), jnp.float32)] * PARTS,
        compiler_params=MIDDLE,
        name="block",
    )(part, core, image, *xs, *weights)


def finish_kernel(part_ref, r0, r1, r2, r3, out_ref, pooled_ref, out_vmem, sems):
    size = PART_SLOTS * TILE
    halo = ROWS_W - size
    received = (r0, r1, r2, r3)
    writes = []
    pooled = jnp.zeros((IMG, PW), jnp.float32)
    for d, r in enumerate(received):
        p = (part_ref[0] + PARTS - d) % PARTS
        base = pl.multiple_of(p * size, size)
        before = received[(d + 1) % PARTS][size:ROWS_W, :]
        start = r[:halo, :] + jnp.where(p > 0, before, jnp.zeros_like(before))
        out_vmem[pl.ds(base, halo), :] = start
        out_vmem[pl.ds(pl.multiple_of(base + halo, TILE), size - halo), :] = r[halo:size, :]
        rows = pl.ds(base, size)
        writes.append(pltpu.make_async_copy(out_vmem.at[rows, :], out_ref.at[rows, :], sems.at[d]))
        writes[-1].start()
        for n in range(3):
            pooled = pooled + r[ROWS_W + n * IMG : ROWS_W + (n + 1) * IMG, :].astype(jnp.float32)
    pooled_ref[...] = pooled
    for write in writes:
        write.wait()


def finish(part, received):
    return pl.pallas_call(
        finish_kernel,
        grid_spec=pltpu.PrefetchScalarGridSpec(
            num_scalar_prefetch=1,
            grid=(1,),
            in_specs=[pl.BlockSpec(memory_space=pltpu.VMEM)] * PARTS,
            out_specs=[pl.BlockSpec(memory_space=pl.ANY), pl.BlockSpec((IMG, PW), lambda i, a: (0, 0))],
            scratch_shapes=[
                pltpu.VMEM((SLOTS * TILE, PW), jnp.bfloat16),
                pltpu.SemaphoreType.DMA((PARTS,)),
            ],
        ),
        out_shape=[
            jax.ShapeDtypeStruct((SLOTS * TILE, PW), jnp.bfloat16),
            jax.ShapeDtypeStruct((IMG, PW), jnp.float32),
        ],
        compiler_params=VMEM,
        name="finish",
    )(part, *received)


def pool_kernel(sums_ref, number_ref, pooled_ref, image_ref, out_ref):
    total = jnp.sum(sums_ref[...], axis=0)
    centre = jnp.concatenate([total[0:1], total[1:2]], axis=1) / number_ref[0:1, 0:1]
    slots = lax.broadcasted_iota(jnp.int32, (IMG, SLOTS), 0) == image_ref[...]
    present = jnp.max(jnp.where(slots, 1.0, 0.0), axis=1, keepdims=True) > 0.5
    out_ref[...] = jnp.where(present, pooled_ref[...] - centre, 0.0).astype(jnp.bfloat16)


def pool(sums, number, pooled, image):
    return pl.pallas_call(
        pool_kernel,
        in_specs=[pl.BlockSpec(memory_space=pltpu.VMEM)] * 4,
        out_shape=jax.ShapeDtypeStruct((IMG, PW), jnp.bfloat16),
        name="pool",
    )(sums, number, pooled, image)


def passed_on(pieces, shift):
    got = []
    for d in (1, 2, 3):
        got.append(lax.ppermute(pieces[d], "mp", shift(d)))
    return got


def whole_block(patches, dest_owner, dest_slot, packed_image, w_query, w_key, w_value, w_out):
    senders = lax.axis_size("dp")
    splits = lax.axis_size("mp")
    part = lax.axis_index("mp").astype(jnp.int32).reshape(1)
    core = (lax.axis_index("dp").astype(jnp.int32) & 1).reshape(1)
    near = lambda array: pltpu.with_memory_space_constraint(array, pltpu.VMEM)
    far = lambda array: pltpu.with_memory_space_constraint(array, pltpu.HBM)
    shift = lambda d: [(i, (i + d) % splits) for i in range(splits)]
    swap = [(i, i ^ 1) for i in range(senders)]

    own = (w_query, w_key, w_value, w_out)
    image = packed_image.reshape(1, SLOTS)
    outgoing, s0, s1 = send_pack(dest_owner, dest_slot, part, core, image, patches, own, senders)
    a0, a1 = (lax.ppermute(s, "mp", shift(1)) for s in (s0, s1))
    b0, b1 = (lax.ppermute(s, "mp", shift(-1)) for s in (s0, s1))
    c0 = lax.ppermute(a0, "mp", shift(1))
    c1 = lax.ppermute(b1, "mp", shift(-1))
    a0x, a1x, b0x, b1x, c0x, c1x = (lax.ppermute(w, "dp", swap) for w in (a0, a1, b0, b1, c0, c1))
    weights = own + (a0, a1, a0x, a1x, b0, b1, b0x, b1x, c0, c1, c0x, c1x)

    incoming = lax.all_to_all(outgoing, "dp", split_axis=0, concat_axis=0, tiled=True)
    *windows, number = arrive_sort(part, near(incoming))
    rows = [windows[0]] + passed_on(windows, shift)
    outcome = block(part, core, packed_image, [near(r) for r in rows], [far(w) for w in weights])
    results, sums = outcome[:PARTS], outcome[PARTS:]
    total = sums[0] + sum(lax.ppermute(sums[d], "mp", shift(d)) for d in (1, 2, 3))
    received = [results[0]] + passed_on(results, shift)
    spread = jnp.broadcast_to(total[None], (senders, 2, PW // 2))
    gathered = lax.all_to_all(spread, "dp", split_axis=0, concat_axis=0, tiled=True)
    packed_out, pooled = finish(part, [near(r) for r in received])
    pooled_out = pool(near(gathered), number, pooled, image)
    return (packed_out, pooled_out)


def solution(mesh):
    in_specs = (
        P("dp", None),
        P("dp"),
        P("dp"),
        P("dp"),
        P(None, "mp"),
        P(None, "mp"),
        P(None, "mp"),
        P("mp", None),
    )
    out_specs = (P("dp", "mp"), P("dp", "mp"))
    return jax.shard_map(whole_block, mesh=mesh, in_specs=in_specs, out_specs=out_specs, check_vma=False)
```

```python
import jax
import jax.numpy as jnp
from jax import lax
from jax.experimental import pallas as pl
from jax.experimental.pallas import tpu as pltpu
from jax.sharding import PartitionSpec as P

EPSILON = 1e-06
SLOTS = 128
TILE = 16
D = 1024
PARTS = 4
PW = D // PARTS
PART_SLOTS = SLOTS // PARTS
WIN = PART_SLOTS + 15
ROWS_W = WIN * TILE
IMG = 16
EXTRA = 3 * IMG
HD = 64
MAX_LOCAL = 4
PAY = 72
EXP_SCALE = HD ** (-0.5) * 1.4426950408889634
VMEM = pltpu.CompilerParams(vmem_limit_bytes=56 * 1024 * 1024)
MIDDLE = pltpu.CompilerParams(vmem_limit_bytes=32 * 1024 * 1024)
SMALL = pltpu.CompilerParams(vmem_limit_bytes=16 * 1024 * 1024)


def send_kernel(owner_ref, slot_ref, mp_ref, core_ref, image_ref, patch_ref, wq, wk, wv, wo, out_ref, s0, s1, count_ref, place_ref, sems):
    owners = out_ref.shape[0]
    core = core_ref[0]
    even = [pltpu.make_async_copy(wq, s0, sems.at[0]), pltpu.make_async_copy(wk, s1, sems.at[1])]
    odd = [pltpu.make_async_copy(wv, s0, sems.at[0])]
    for n in range(PARTS):
        block_rows = pl.ds(n * PW, PW)
        odd.append(pltpu.make_async_copy(wo.at[:, block_rows], s1.at[block_rows, :], sems.at[1 + n]))

    @pl.when(core == 0)
    def _():
        for copy in even:
            copy.start()

    @pl.when(core != 0)
    def _():
        for copy in odd:
            copy.start()

    def clear(o, carry):
        count_ref[o] = 0
        return carry

    lax.fori_loop(0, owners, clear, 0, unroll=8)

    def move(t, carry):
        o = owner_ref[t]
        r = count_ref[o]
        count_ref[o] = r + 1
        place_ref[2 * o + r] = slot_ref[t]
        rows = patch_ref[pl.ds(pl.multiple_of(t * TILE, TILE), TILE), :]
        base = pl.multiple_of(r * 2 * TILE, TILE)
        out_ref[o, pl.ds(base, TILE), :] = rows[:, :128]
        out_ref[o, pl.ds(base + TILE, TILE), :] = rows[:, 128:]
        return carry

    lax.fori_loop(0, SLOTS, move, 0, unroll=8)
    row = lax.broadcasted_iota(jnp.int32, (PAY - 64, 128), 0)
    images = jnp.max(image_ref[...], axis=1, keepdims=True) + 1
    images = jnp.broadcast_to(images, row.shape)

    def label(o, carry):
        value = jnp.where(row == 0, place_ref[2 * o], jnp.where(row == 1, place_ref[2 * o + 1], images))
        out_ref[o, 64:, :] = value.astype(jnp.float32).astype(jnp.bfloat16)
        return carry

    lax.fori_loop(0, owners, label, 0, unroll=8)

    @pl.when(core == 0)
    def _():
        for copy in even:
            copy.wait()

    @pl.when(core != 0)
    def _():
        for copy in odd:
            copy.wait()


def send_pack(owner, slot, part, core, image, patches, weights, senders):
    return pl.pallas_call(
        send_kernel,
        grid_spec=pltpu.PrefetchScalarGridSpec(
            num_scalar_prefetch=4,
            grid=(1,),
            in_specs=[
                pl.BlockSpec((1, SLOTS), lambda i, a, b, m, c: (0, 0)),
                pl.BlockSpec((SLOTS * TILE, PW), lambda i, a, b, m, c: (0, m[0])),
            ]
            + [pl.BlockSpec(memory_space=pl.ANY)] * 4,
            out_specs=[pl.BlockSpec((senders, PAY, 128), lambda i, a, b, m, c: (0, 0, 0))]
            + [pl.BlockSpec((D, PW), lambda i, a, b, m, c: (0, 0))] * 2,
            scratch_shapes=[
                pltpu.SMEM((senders,), jnp.int32),
                pltpu.SMEM((2 * senders,), jnp.int32),
                pltpu.SemaphoreType.DMA((1 + PARTS,)),
            ],
        ),
        out_shape=[jax.ShapeDtypeStruct((senders, PAY, 128), jnp.bfloat16)]
        + [jax.ShapeDtypeStruct((D, PW), jnp.bfloat16)] * 2,
        compiler_params=VMEM,
        name="send_pack",
    )(owner, slot, part, core, image, patches, *weights)


def arrive_kernel(mp_ref, in_ref, out0, out1, out2, out3, total_ref, sorted_ref, label_ref, slot_ref, sem):
    senders = in_ref.shape[0]
    row = lax.broadcasted_iota(jnp.int32, (8, 128), 0)
    lane = lax.broadcasted_iota(jnp.int32, (8, 128), 1)
    picked = jnp.zeros((8, 128), jnp.float32)
    total = jnp.zeros((8, 128), jnp.float32)
    for s in range(senders):
        marks = in_ref[s, 64:, :].astype(jnp.float32)
        picked = jnp.where((lane == 2 * s) | (lane == 2 * s + 1), marks, picked)
        total = total + marks
    odd = (lane & 1) == 1
    own = jnp.where(row == jnp.where(odd, 1, 0), picked, 0.0)
    label_ref[...] = jnp.broadcast_to(jnp.sum(own, axis=0, keepdims=True), (8, 128)).astype(jnp.int32)
    copy = pltpu.make_async_copy(label_ref, slot_ref, sem)
    copy.start()
    total_ref[...] = jnp.broadcast_to(jnp.sum(jnp.where(row == 2, total, 0.0), axis=0, keepdims=True), (8, 128))
    sorted_ref[SLOTS * TILE :, :] = jnp.zeros((ROWS_W - PART_SLOTS * TILE, PW), jnp.bfloat16)
    copy.wait()

    def move(s, carry):
        for r in range(2):
            at = pl.multiple_of(slot_ref[0, 2 * s + r] * TILE, TILE)
            sorted_ref[pl.ds(at, TILE), :128] = in_ref[s, 2 * r * TILE : (2 * r + 1) * TILE, :]
            sorted_ref[pl.ds(at, TILE), 128:] = in_ref[s, (2 * r + 1) * TILE : (2 * r + 2) * TILE, :]
        return carry

    lax.fori_loop(0, senders, move, 0, unroll=8)
    for d, out in enumerate((out0, out1, out2, out3)):
        part = (mp_ref[0] + d) % PARTS
        at = pl.multiple_of(part * PART_SLOTS * TILE, TILE)
        out[...] = sorted_ref[pl.ds(at, ROWS_W), :]


def arrive_sort(mp, incoming):
    window = jax.ShapeDtypeStruct((ROWS_W, PW), jnp.bfloat16)
    return pl.pallas_call(
        arrive_kernel,
        grid_spec=pltpu.PrefetchScalarGridSpec(
            num_scalar_prefetch=1,
            grid=(1,),
            in_specs=[pl.BlockSpec(memory_space=pltpu.VMEM)],
            out_specs=[pl.BlockSpec(memory_space=pltpu.VMEM)] * (PARTS + 1),
            scratch_shapes=[
                pltpu.VMEM((SLOTS * TILE + ROWS_W - PART_SLOTS * TILE, PW), jnp.bfloat16),
                pltpu.VMEM((8, 128), jnp.int32),
                pltpu.SMEM((8, 128), jnp.int32),
                pltpu.SemaphoreType.DMA,
            ],
        ),
        out_shape=[window] * PARTS + [jax.ShapeDtypeStruct((8, 128), jnp.float32)],
        compiler_params=SMALL,
        name="arrive_sort",
    )(mp, incoming)


def block_kernel(part_ref, core_ref, image_ref, x0, x1, x2, x3, wq, wk, wv, wo, a0, a1, a0x, a1x, b0, b1, b0x, b1x, c0, c1, c0x, c1x,
                 out0, out1, out2, out3, sum0, sum1, sum2, sum3,
                 norm_ref, q_ref, k_ref, v_ref, att_ref, w_refs, begin_ref, end_ref, wsem):
    part = part_ref[0]
    core = core_ref[0]
    xs = (x0, x1, x2, x3)
    copies = [[pltpu.make_async_copy(w, w_refs.at[0, n], wsem.at[n]) for n, w in enumerate((wq, wk, wv))]]
    for n in range(PARTS):
        block_rows = pl.ds(n * PW, PW)
        copies[0].append(pltpu.make_async_copy(wo.at[:, block_rows], w_refs.at[0, 3, block_rows, :], wsem.at[4 * PARTS - 1 + n]))
    for g, (m0, m1, o0, o1) in enumerate(((a0, a1, a0x, a1x), (b0, b1, b0x, b1x), (c0, c1, c0x, c1x))):
        group = []
        for n, (w, place) in enumerate(((m0, 2 * core), (m1, 2 * core + 1), (o0, 2 - 2 * core), (o1, 3 - 2 * core))):
            group.append(pltpu.make_async_copy(w, w_refs.at[g + 1, place], wsem.at[4 * g + 3 + n]))
        copies.append(group)
    for group in copies:
        for copy in group:
            copy.start()

    window = part * PART_SLOTS
    for i in range(8):
        begin_ref[i] = 0
        end_ref[i] = 0

    def scan(l, carry):
        before, count, first, mine = carry
        t = window + l
        label = jnp.where(t < SLOTS, image_ref[jnp.minimum(t, SLOTS - 1)], -1)
        fresh = (label >= 0) & (label != before)
        starts = fresh & (l < PART_SLOTS)
        mine = jnp.where(fresh, jnp.where(starts, 1, 0), jnp.where(label >= 0, mine, 0))
        first = jnp.where(starts & (count == 0), label, first)
        count = count + jnp.where(starts, 1, 0)
        begin_ref[jnp.where(starts, count - 1, 7)] = l
        end_ref[jnp.where(mine == 1, count - 1, 7)] = l + 1
        return label, count, first, mine

    before = jnp.where(part > 0, image_ref[jnp.maximum(window - 1, 0)], -1)
    _, count, first, _ = lax.fori_loop(0, WIN + 1, scan, (before, jnp.int32(0), jnp.int32(0), jnp.int32(0)), unroll=4)

    chunk = 128

    def norm(i, carry):
        at = pl.multiple_of(jnp.minimum(i * chunk, ROWS_W - chunk), TILE)
        rows = [x[pl.ds(at, chunk), :].astype(jnp.float32) for x in xs]
        mean = jnp.sum(rows[0] + rows[1] + rows[2] + rows[3], axis=-1, keepdims=True) * (1.0 / D)
        centred = [r - mean for r in rows]
        squares = [r * r for r in centred]
        spread = jnp.sum(squares[0] + squares[1] + squares[2] + squares[3], axis=-1, keepdims=True) * (1.0 / D)
        scale = lax.rsqrt(spread + EPSILON)
        for d in range(PARTS):
            norm_ref[(part + PARTS - d) % PARTS, pl.ds(at, chunk), :] = (centred[d] * scale).astype(jnp.bfloat16)
        return carry

    lax.fori_loop(0, pl.cdiv(ROWS_W, chunk), norm, 0)

    for g in range(PARTS):
        for copy in copies[g]:
            copy.wait()
        for n, ref in enumerate((q_ref, k_ref, v_ref)):
            normed = jnp.concatenate([norm_ref[p] for p in range(PARTS)], axis=1)
            ref[...] = jnp.dot(normed, w_refs[g, n], preferred_element_type=jnp.float32).astype(jnp.bfloat16)

        def image(i, carry):
            row = pl.multiple_of(begin_ref[i] * TILE, TILE)
            limit = (end_ref[i] - begin_ref[i]) * TILE

            def mix(size):
                window = pl.ds(row, size)
                queries = q_ref[window, :]
                keys = k_ref[window, :]
                values = v_ref[window, :]
                allowed = lax.broadcasted_iota(jnp.int32, (size, size - 128), 1) + 128 < limit
                lane = lax.broadcasted_iota(jnp.int32, (size, PW), 1)
                low = lax.broadcasted_iota(jnp.int32, (size, 128), 1) < HD
                heads = range(PW // HD)
                inside = [(lane >= h * HD) & (lane < (h + 1) * HD) for h in heads]
                nears, fars = [], []
                scores = [
                    lax.dot_general(queries, jnp.where(inside[h], keys, jnp.zeros_like(keys)), (((1,), (1,)), ((), ())), preferred_element_type=jnp.float32)
                    for h in heads
                ]
                raised = []
                for h in heads:
                    always, maybe = scores[h][:, :128], jnp.where(allowed, scores[h][:, 128:], -1e30)
                    peak = jnp.maximum(jnp.max(always, axis=-1, keepdims=True), jnp.max(maybe, axis=-1, keepdims=True))
                    raised.append(jnp.exp2((jnp.concatenate([always, maybe], axis=1) - peak) * EXP_SCALE).astype(jnp.bfloat16))
                for h in heads:
                    mixed = jnp.dot(raised[h], jnp.where(inside[h], values, jnp.ones_like(values)), preferred_element_type=jnp.float32)
                    near, far = (mixed[:, :128], mixed[:, 128:]) if h < 2 else (mixed[:, 128:], mixed[:, :128])
                    nears.append(near)
                    fars.append(far)
                for half in range(2):
                    top = jnp.where(low, nears[2 * half], nears[2 * half + 1])
                    bottom = jnp.where(low, fars[2 * half], fars[2 * half + 1])
                    att_ref[window, g * PW + half * 128 : g * PW + (half + 1) * 128] = (top / bottom).astype(jnp.bfloat16)

            @pl.when(limit <= 192)
            def _():
                mix(192)

            @pl.when(limit > 192)
            def _():
                mix(256)

            return carry

        lax.fori_loop(0, count, image, 0)

    start_row = begin_ref[0] * TILE
    end_row = end_ref[0]
    for i in range(1, MAX_LOCAL):
        end_row = jnp.maximum(end_row, end_ref[i])
    end_row = end_row * TILE
    row_ids = lax.broadcasted_iota(jnp.int32, (ROWS_W, PW), 0)
    live = (row_ids >= start_row) & (row_ids < end_row)
    tile_ids = lax.broadcasted_iota(jnp.int32, (WIN, 8, PW), 0)
    pooled_ids = lax.broadcasted_iota(jnp.int32, (IMG, PW), 0)
    lengths = jnp.ones((IMG, PW), jnp.float32)
    tiles = []
    for i in range(MAX_LOCAL):
        tiles.append((tile_ids >= begin_ref[i]) & (tile_ids < end_ref[i]))
        rows_i = ((end_ref[i] - begin_ref[i]) * TILE).astype(jnp.float32)
        lengths = jnp.where((pooled_ids == first + i) & (rows_i > 0), rows_i, lengths)
    for d, (out, sum_ref) in enumerate(((out0, sum0), (out1, sum1), (out2, sum2), (out3, sum3))):
        n = (part + d) % PARTS
        block_rows = pl.ds(pl.multiple_of(n * PW, PW), PW)
        mix = jnp.concatenate([w_refs[g, 3, block_rows, :] for g in range(PARTS)], axis=0)
        projected = jnp.dot(att_ref[...], mix, preferred_element_type=jnp.float32)
        result = jnp.where(live, xs[-d % PARTS][...].astype(jnp.float32) + projected, 0.0)
        out[:ROWS_W, :] = result.astype(jnp.bfloat16)
        pairs = result.reshape(WIN, 2, 8, PW)
        pairs = pairs[:, 0] + pairs[:, 1]
        sums = jnp.zeros((IMG, PW), jnp.float32)
        for i in range(MAX_LOCAL):
            held = jnp.sum(jnp.where(tiles[i], pairs, 0.0), axis=0)
            sums = jnp.where(pooled_ids == first + i, jnp.sum(held, axis=0, keepdims=True), sums)
        pooled = sums / lengths
        one = pooled.astype(jnp.bfloat16)
        rest = pooled - one.astype(jnp.float32)
        two = rest.astype(jnp.bfloat16)
        three = (rest - two.astype(jnp.float32)).astype(jnp.bfloat16)
        out[ROWS_W : ROWS_W + IMG, :] = one
        out[ROWS_W + IMG : ROWS_W + 2 * IMG, :] = two
        out[ROWS_W + 2 * IMG : ROWS_W + 3 * IMG, :] = three
        line = jnp.sum(pooled, axis=0, keepdims=True)
        sum_ref[0:1, :] = line[:, : PW // 2]
        sum_ref[1:2, :] = line[:, PW // 2 :]


def block(part, core, image, xs, weights):
    outs = jax.ShapeDtypeStruct((ROWS_W + EXTRA, PW), jnp.bfloat16)
    wide = pltpu.VMEM((ROWS_W, PW), jnp.bfloat16)
    return pl.pallas_call(
        block_kernel,
        grid_spec=pltpu.PrefetchScalarGridSpec(
            num_scalar_prefetch=3,
            grid=(1,),
            in_specs=[pl.BlockSpec(memory_space=pltpu.VMEM)] * len(xs)
            + [pl.BlockSpec(memory_space=pltpu.HBM)] * len(weights),
            out_specs=[pl.BlockSpec(memory_space=pltpu.VMEM)] * (2 * PARTS),
            scratch_shapes=[
                pltpu.VMEM((PARTS, ROWS_W, PW), jnp.bfloat16),
                wide,
                wide,
                wide,
                pltpu.VMEM((ROWS_W, D), jnp.bfloat16),
                pltpu.VMEM((PARTS, 4, D, PW), jnp.bfloat16),
                pltpu.SMEM((8,), jnp.int32),
                pltpu.SMEM((8,), jnp.int32),
                pltpu.SemaphoreType.DMA((5 * PARTS - 1,)),
            ],
        ),
        out_shape=[outs] * PARTS + [jax.ShapeDtypeStruct((2, PW // 2), jnp.float32)] * PARTS,
        compiler_params=MIDDLE,
        name="block",
    )(part, core, image, *xs, *weights)


def finish_kernel(part_ref, r0, r1, r2, r3, out_ref, pooled_ref, out_vmem, sems):
    size = PART_SLOTS * TILE
    halo = ROWS_W - size
    received = (r0, r1, r2, r3)
    writes = []
    pooled = jnp.zeros((IMG, PW), jnp.float32)
    for d, r in enumerate(received):
        p = (part_ref[0] + PARTS - d) % PARTS
        base = pl.multiple_of(p * size, size)
        before = received[(d + 1) % PARTS][size:ROWS_W, :]
        start = r[:halo, :] + jnp.where(p > 0, before, jnp.zeros_like(before))
        out_vmem[pl.ds(base, halo), :] = start
        out_vmem[pl.ds(pl.multiple_of(base + halo, TILE), size - halo), :] = r[halo:size, :]
        rows = pl.ds(base, size)
        writes.append(pltpu.make_async_copy(out_vmem.at[rows, :], out_ref.at[rows, :], sems.at[d]))
        writes[-1].start()
        for n in range(3):
            pooled = pooled + r[ROWS_W + n * IMG : ROWS_W + (n + 1) * IMG, :].astype(jnp.float32)
    pooled_ref[...] = pooled
    for write in writes:
        write.wait()


def finish(part, received):
    return pl.pallas_call(
        finish_kernel,
        grid_spec=pltpu.PrefetchScalarGridSpec(
            num_scalar_prefetch=1,
            grid=(1,),
            in_specs=[pl.BlockSpec(memory_space=pltpu.VMEM)] * PARTS,
            out_specs=[pl.BlockSpec(memory_space=pl.ANY), pl.BlockSpec((IMG, PW), lambda i, a: (0, 0))],
            scratch_shapes=[
                pltpu.VMEM((SLOTS * TILE, PW), jnp.bfloat16),
                pltpu.SemaphoreType.DMA((PARTS,)),
            ],
        ),
        out_shape=[
            jax.ShapeDtypeStruct((SLOTS * TILE, PW), jnp.bfloat16),
            jax.ShapeDtypeStruct((IMG, PW), jnp.float32),
        ],
        compiler_params=VMEM,
        name="finish",
    )(part, *received)


def pool_kernel(sums_ref, number_ref, pooled_ref, image_ref, out_ref):
    total = jnp.sum(sums_ref[...], axis=0)
    centre = jnp.concatenate([total[0:1], total[1:2]], axis=1) / number_ref[0:1, 0:1]
    slots = lax.broadcasted_iota(jnp.int32, (IMG, SLOTS), 0) == image_ref[...]
    present = jnp.max(jnp.where(slots, 1.0, 0.0), axis=1, keepdims=True) > 0.5
    out_ref[...] = jnp.where(present, pooled_ref[...] - centre, 0.0).astype(jnp.bfloat16)


def pool(sums, number, pooled, image):
    return pl.pallas_call(
        pool_kernel,
        in_specs=[pl.BlockSpec(memory_space=pltpu.VMEM)] * 4,
        out_shape=jax.ShapeDtypeStruct((IMG, PW), jnp.bfloat16),
        name="pool",
    )(sums, number, pooled, image)


def passed_on(pieces, shift):
    got = []
    for d in (1, 2, 3):
        got.append(lax.ppermute(pieces[d], "mp", shift(d)))
    return got


def whole_block(patches, dest_owner, dest_slot, packed_image, w_query, w_key, w_value, w_out):
    senders = lax.axis_size("dp")
    splits = lax.axis_size("mp")
    part = lax.axis_index("mp").astype(jnp.int32).reshape(1)
    core = (lax.axis_index("dp").astype(jnp.int32) & 1).reshape(1)
    near = lambda array: pltpu.with_memory_space_constraint(array, pltpu.VMEM)
    far = lambda array: pltpu.with_memory_space_constraint(array, pltpu.HBM)
    shift = lambda d: [(i, (i + d) % splits) for i in range(splits)]
    swap = [(i, i ^ 1) for i in range(senders)]

    own = (w_query, w_key, w_value, w_out)
    image = packed_image.reshape(1, SLOTS)
    outgoing, s0, s1 = send_pack(dest_owner, dest_slot, part, core, image, patches, own, senders)
    a0 = lax.ppermute(s0, "mp", shift(1))
    b1 = lax.ppermute(s1, "mp", shift(-1))
    a1 = lax.ppermute(s1, "mp", shift(1))
    b0 = lax.ppermute(s0, "mp", shift(-1))
    c0 = lax.ppermute(a0, "mp", shift(1))
    c1 = lax.ppermute(b1, "mp", shift(-1))
    a0x, a1x, b0x, b1x, c0x, c1x = (lax.ppermute(w, "dp", swap) for w in (a0, a1, b0, b1, c0, c1))
    weights = own + (a0, a1, a0x, a1x, b0, b1, b0x, b1x, c0, c1, c0x, c1x)

    incoming = lax.all_to_all(outgoing, "dp", split_axis=0, concat_axis=0, tiled=True)
    *windows, number = arrive_sort(part, near(incoming))
    rows = [windows[0]] + passed_on(windows, shift)
    outcome = block(part, core, packed_image, [near(r) for r in rows], [far(w) for w in weights])
    results, sums = outcome[:PARTS], outcome[PARTS:]
    total = sums[0] + sum(lax.ppermute(sums[d], "mp", shift(d)) for d in (1, 2, 3))
    received = [results[0]] + passed_on(results, shift)
    spread = jnp.broadcast_to(total[None], (senders, 2, PW // 2))
    gathered = lax.all_to_all(spread, "dp", split_axis=0, concat_axis=0, tiled=True)
    packed_out, pooled = finish(part, [near(r) for r in received])
    pooled_out = pool(near(gathered), number, pooled, image)
    return (packed_out, pooled_out)


def solution(mesh):
    in_specs = (
        P("dp", None),
        P("dp"),
        P("dp"),
        P("dp"),
        P(None, "mp"),
        P(None, "mp"),
        P(None, "mp"),
        P("mp", None),
    )
    out_specs = (P("dp", "mp"), P("dp", "mp"))
    return jax.shard_map(whole_block, mesh=mesh, in_specs=in_specs, out_specs=out_specs, check_vma=False)
```

```python
import jax
import jax.numpy as jnp
from jax import lax
from jax.experimental import pallas as pl
from jax.experimental.pallas import tpu as pltpu
from jax.sharding import PartitionSpec as P

EPSILON = 1e-06
SLOTS = 128
TILE = 16
D = 1024
PARTS = 4
PW = D // PARTS
PART_SLOTS = SLOTS // PARTS
WIN = PART_SLOTS + 15
ROWS_W = WIN * TILE
IMG = 16
EXTRA = TILE
HD = 64
MAX_LOCAL = 4
PAY = 72
EXP_SCALE = HD ** (-0.5) * 1.4426950408889634
VMEM = pltpu.CompilerParams(vmem_limit_bytes=56 * 1024 * 1024)
MIDDLE = pltpu.CompilerParams(vmem_limit_bytes=32 * 1024 * 1024)
SMALL = pltpu.CompilerParams(vmem_limit_bytes=16 * 1024 * 1024)


def send_kernel(owner_ref, slot_ref, mp_ref, core_ref, image_ref, patch_ref, wq, wk, wv, wo, out_ref, s0, s1, count_ref, place_ref, rank_ref, rows_ref, sems, row_sems):
    owners = out_ref.shape[0]
    core = core_ref[0]
    chunk = SLOTS * TILE // PARTS
    own_columns = pl.ds(pl.multiple_of(mp_ref[0] * PW, PW), PW)
    fetches = []
    for n in range(PARTS):
        some = pl.ds(n * chunk, chunk)
        fetches.append(pltpu.make_async_copy(patch_ref.at[some, own_columns], rows_ref.at[some, :], row_sems.at[n]))
        fetches[-1].start()
    even = [pltpu.make_async_copy(wq, s0, sems.at[0]), pltpu.make_async_copy(wk, s1, sems.at[1])]
    odd = [pltpu.make_async_copy(wv, s0, sems.at[0])]
    for n in range(PARTS):
        block_rows = pl.ds(n * PW, PW)
        odd.append(pltpu.make_async_copy(wo.at[:, block_rows], s1.at[block_rows, :], sems.at[1 + n]))

    @pl.when(core == 0)
    def _():
        for copy in even:
            copy.start()

    @pl.when(core != 0)
    def _():
        for copy in odd:
            copy.start()

    def clear(o, carry):
        count_ref[o] = 0
        return carry

    lax.fori_loop(0, owners, clear, 0, unroll=8)

    def rank(t, carry):
        o = owner_ref[t]
        r = count_ref[o]
        count_ref[o] = r + 1
        place_ref[2 * o + r] = slot_ref[t]
        rank_ref[t] = r
        return carry

    lax.fori_loop(0, SLOTS, rank, 0, unroll=8)
    row = lax.broadcasted_iota(jnp.int32, (PAY - 64, 128), 0)
    images = jnp.max(image_ref[...], axis=1, keepdims=True) + 1
    images = jnp.broadcast_to(images, row.shape)

    def label(o, carry):
        value = jnp.where(row == 0, place_ref[2 * o], jnp.where(row == 1, place_ref[2 * o + 1], images))
        out_ref[o, 64:, :] = value.astype(jnp.float32).astype(jnp.bfloat16)
        return carry

    lax.fori_loop(0, owners, label, 0, unroll=8)

    def move(t, carry):
        o = owner_ref[t]
        rows = rows_ref[pl.ds(pl.multiple_of(t * TILE, TILE), TILE), :]
        base = pl.multiple_of(rank_ref[t] * 2 * TILE, TILE)
        out_ref[o, pl.ds(base, TILE), :] = rows[:, :128]
        out_ref[o, pl.ds(base + TILE, TILE), :] = rows[:, 128:]
        return carry

    for n in range(PARTS):
        fetches[n].wait()
        lax.fori_loop(n * SLOTS // PARTS, (n + 1) * SLOTS // PARTS, move, 0, unroll=8)

    @pl.when(core == 0)
    def _():
        for copy in even:
            copy.wait()

    @pl.when(core != 0)
    def _():
        for copy in odd:
            copy.wait()


def send_pack(owner, slot, part, core, image, patches, weights, senders):
    return pl.pallas_call(
        send_kernel,
        grid_spec=pltpu.PrefetchScalarGridSpec(
            num_scalar_prefetch=4,
            grid=(1,),
            in_specs=[
                pl.BlockSpec((1, SLOTS), lambda i, a, b, m, c: (0, 0)),
            ]
            + [pl.BlockSpec(memory_space=pl.ANY)] * 5,
            out_specs=[pl.BlockSpec((senders, PAY, 128), lambda i, a, b, m, c: (0, 0, 0))]
            + [pl.BlockSpec((D, PW), lambda i, a, b, m, c: (0, 0))] * 2,
            scratch_shapes=[
                pltpu.SMEM((senders,), jnp.int32),
                pltpu.SMEM((2 * senders,), jnp.int32),
                pltpu.SMEM((SLOTS,), jnp.int32),
                pltpu.VMEM((SLOTS * TILE, PW), jnp.bfloat16),
                pltpu.SemaphoreType.DMA((1 + PARTS,)),
                pltpu.SemaphoreType.DMA((PARTS,)),
            ],
        ),
        out_shape=[jax.ShapeDtypeStruct((senders, PAY, 128), jnp.bfloat16)]
        + [jax.ShapeDtypeStruct((D, PW), jnp.bfloat16)] * 2,
        compiler_params=VMEM,
        name="send_pack",
    )(owner, slot, part, core, image, patches, *weights)


def arrive_kernel(mp_ref, in_ref, out0, out1, out2, out3, total_ref, sorted_ref, label_ref, slot_ref, sem):
    senders = in_ref.shape[0]
    row = lax.broadcasted_iota(jnp.int32, (8, 128), 0)
    lane = lax.broadcasted_iota(jnp.int32, (8, 128), 1)
    picked = jnp.zeros((8, 128), jnp.float32)
    total = jnp.zeros((8, 128), jnp.float32)
    for s in range(senders):
        marks = in_ref[s, 64:, :].astype(jnp.float32)
        picked = jnp.where((lane == 2 * s) | (lane == 2 * s + 1), marks, picked)
        total = total + marks
    odd = (lane & 1) == 1
    own = jnp.where(row == jnp.where(odd, 1, 0), picked, 0.0)
    label_ref[...] = jnp.broadcast_to(jnp.sum(own, axis=0, keepdims=True), (8, 128)).astype(jnp.int32)
    copy = pltpu.make_async_copy(label_ref, slot_ref, sem)
    copy.start()
    total_ref[...] = jnp.broadcast_to(jnp.sum(jnp.where(row == 2, total, 0.0), axis=0, keepdims=True), (8, 128))
    sorted_ref[SLOTS * TILE :, :] = jnp.zeros((ROWS_W - PART_SLOTS * TILE, PW), jnp.bfloat16)
    copy.wait()

    def move(s, carry):
        for r in range(2):
            at = pl.multiple_of(slot_ref[0, 2 * s + r] * TILE, TILE)
            sorted_ref[pl.ds(at, TILE), :128] = in_ref[s, 2 * r * TILE : (2 * r + 1) * TILE, :]
            sorted_ref[pl.ds(at, TILE), 128:] = in_ref[s, (2 * r + 1) * TILE : (2 * r + 2) * TILE, :]
        return carry

    lax.fori_loop(0, senders, move, 0, unroll=8)
    for d, out in enumerate((out0, out1, out2, out3)):
        part = (mp_ref[0] + d) % PARTS
        at = pl.multiple_of(part * PART_SLOTS * TILE, TILE)
        out[...] = sorted_ref[pl.ds(at, ROWS_W), :]


def arrive_sort(mp, incoming):
    window = jax.ShapeDtypeStruct((ROWS_W, PW), jnp.bfloat16)
    return pl.pallas_call(
        arrive_kernel,
        grid_spec=pltpu.PrefetchScalarGridSpec(
            num_scalar_prefetch=1,
            grid=(1,),
            in_specs=[pl.BlockSpec(memory_space=pltpu.VMEM)],
            out_specs=[pl.BlockSpec(memory_space=pltpu.VMEM)] * (PARTS + 1),
            scratch_shapes=[
                pltpu.VMEM((SLOTS * TILE + ROWS_W - PART_SLOTS * TILE, PW), jnp.bfloat16),
                pltpu.VMEM((8, 128), jnp.int32),
                pltpu.SMEM((8, 128), jnp.int32),
                pltpu.SemaphoreType.DMA,
            ],
        ),
        out_shape=[window] * PARTS + [jax.ShapeDtypeStruct((8, 128), jnp.float32)],
        compiler_params=SMALL,
        name="arrive_sort",
    )(mp, incoming)


def block_kernel(part_ref, core_ref, image_ref, x0, x1, x2, x3, wq, wk, wv, wo, a0, a1, a0x, a1x, b0, b1, b0x, b1x, c0, c1, c0x, c1x,
                 out0, out1, out2, out3, sum0, sum1, sum2, sum3,
                 norm_ref, q_ref, k_ref, v_ref, att_ref, w_refs, begin_ref, end_ref, wsem):
    part = part_ref[0]
    core = core_ref[0]
    xs = (x0, x1, x2, x3)
    copies = [[pltpu.make_async_copy(w, w_refs.at[0, n], wsem.at[n]) for n, w in enumerate((wq, wk, wv))]]
    for n in range(PARTS):
        block_rows = pl.ds(n * PW, PW)
        copies[0].append(pltpu.make_async_copy(wo.at[:, block_rows], w_refs.at[0, 3, block_rows, :], wsem.at[4 * PARTS - 1 + n]))
    for g, (m0, m1, o0, o1) in enumerate(((a0, a1, a0x, a1x), (b0, b1, b0x, b1x), (c0, c1, c0x, c1x))):
        group = []
        for n, (w, place) in enumerate(((m0, 2 * core), (m1, 2 * core + 1), (o0, 2 - 2 * core), (o1, 3 - 2 * core))):
            group.append(pltpu.make_async_copy(w, w_refs.at[g + 1, place], wsem.at[4 * g + 3 + n]))
        copies.append(group)
    for group in copies:
        for copy in group:
            copy.start()

    window = part * PART_SLOTS
    for i in range(8):
        begin_ref[i] = 0
        end_ref[i] = 0

    def scan(l, carry):
        before, count, first, mine = carry
        t = window + l
        label = jnp.where(t < SLOTS, image_ref[jnp.minimum(t, SLOTS - 1)], -1)
        fresh = (label >= 0) & (label != before)
        starts = fresh & (l < PART_SLOTS)
        mine = jnp.where(fresh, jnp.where(starts, 1, 0), jnp.where(label >= 0, mine, 0))
        first = jnp.where(starts & (count == 0), label, first)
        count = count + jnp.where(starts, 1, 0)
        begin_ref[jnp.where(starts, count - 1, 7)] = l
        end_ref[jnp.where(mine == 1, count - 1, 7)] = l + 1
        return label, count, first, mine

    before = jnp.where(part > 0, image_ref[jnp.maximum(window - 1, 0)], -1)
    _, count, _, _ = lax.fori_loop(0, WIN + 1, scan, (before, jnp.int32(0), jnp.int32(0), jnp.int32(0)), unroll=4)

    chunk = 128

    def norm(i, carry):
        at = pl.multiple_of(jnp.minimum(i * chunk, ROWS_W - chunk), TILE)
        rows = [x[pl.ds(at, chunk), :].astype(jnp.float32) for x in xs]
        mean = jnp.sum(rows[0] + rows[1] + rows[2] + rows[3], axis=-1, keepdims=True) * (1.0 / D)
        centred = [r - mean for r in rows]
        squares = [r * r for r in centred]
        spread = jnp.sum(squares[0] + squares[1] + squares[2] + squares[3], axis=-1, keepdims=True) * (1.0 / D)
        scale = lax.rsqrt(spread + EPSILON)
        for d in range(PARTS):
            norm_ref[(part + PARTS - d) % PARTS, pl.ds(at, chunk), :] = (centred[d] * scale).astype(jnp.bfloat16)
        return carry

    lax.fori_loop(0, pl.cdiv(ROWS_W, chunk), norm, 0)

    for g in range(PARTS):
        for copy in copies[g]:
            copy.wait()
        for n, ref in enumerate((q_ref, k_ref, v_ref)):
            normed = jnp.concatenate([norm_ref[p] for p in range(PARTS)], axis=1)
            ref[...] = jnp.dot(normed, w_refs[g, n], preferred_element_type=jnp.float32).astype(jnp.bfloat16)

        def image(i, carry):
            row = pl.multiple_of(begin_ref[i] * TILE, TILE)
            limit = (end_ref[i] - begin_ref[i]) * TILE

            def mix(size):
                window = pl.ds(row, size)
                queries = q_ref[window, :]
                keys = k_ref[window, :]
                values = v_ref[window, :]
                allowed = lax.broadcasted_iota(jnp.int32, (size, size - 128), 1) + 128 < limit
                lane = lax.broadcasted_iota(jnp.int32, (size, PW), 1)
                low = lax.broadcasted_iota(jnp.int32, (size, 128), 1) < HD
                heads = range(PW // HD)
                inside = [(lane >= h * HD) & (lane < (h + 1) * HD) for h in heads]
                nears, fars = [], []
                scores = [
                    lax.dot_general(queries, jnp.where(inside[h], keys, jnp.zeros_like(keys)), (((1,), (1,)), ((), ())), preferred_element_type=jnp.float32)
                    for h in heads
                ]
                raised = []
                for h in heads:
                    always, maybe = scores[h][:, :128], jnp.where(allowed, scores[h][:, 128:], -1e30)
                    peak = jnp.maximum(jnp.max(always, axis=-1, keepdims=True), jnp.max(maybe, axis=-1, keepdims=True))
                    raised.append(jnp.exp2((jnp.concatenate([always, maybe], axis=1) - peak) * EXP_SCALE).astype(jnp.bfloat16))
                for h in heads:
                    mixed = jnp.dot(raised[h], jnp.where(inside[h], values, jnp.ones_like(values)), preferred_element_type=jnp.float32)
                    near, far = (mixed[:, :128], mixed[:, 128:]) if h < 2 else (mixed[:, 128:], mixed[:, :128])
                    nears.append(near)
                    fars.append(far)
                for half in range(2):
                    top = jnp.where(low, nears[2 * half], nears[2 * half + 1])
                    bottom = jnp.where(low, fars[2 * half], fars[2 * half + 1])
                    att_ref[window, g * PW + half * 128 : g * PW + (half + 1) * 128] = (top / bottom).astype(jnp.bfloat16)

            @pl.when(limit <= 192)
            def _():
                mix(192)

            @pl.when(limit > 192)
            def _():
                mix(256)

            return carry

        lax.fori_loop(0, count, image, 0)

    start_row = begin_ref[0] * TILE
    end_row = end_ref[0]
    for i in range(1, MAX_LOCAL):
        end_row = jnp.maximum(end_row, end_ref[i])
    end_row = end_row * TILE
    row_ids = lax.broadcasted_iota(jnp.int32, (ROWS_W, PW), 0)
    live = (row_ids >= start_row) & (row_ids < end_row)
    tile_ids = lax.broadcasted_iota(jnp.int32, (WIN, 8, PW), 0)
    term_ids = lax.broadcasted_iota(jnp.int32, (EXTRA, PW), 0)
    tiles = [(tile_ids >= begin_ref[i]) & (tile_ids < end_ref[i]) for i in range(MAX_LOCAL)]
    lengths = [jnp.maximum((end_ref[i] - begin_ref[i]) * TILE, 1).astype(jnp.float32) for i in range(MAX_LOCAL)]
    for d, (out, sum_ref) in enumerate(((out0, sum0), (out1, sum1), (out2, sum2), (out3, sum3))):
        n = (part + d) % PARTS
        block_rows = pl.ds(pl.multiple_of(n * PW, PW), PW)
        mix = jnp.concatenate([w_refs[g, 3, block_rows, :] for g in range(PARTS)], axis=0)
        projected = jnp.dot(att_ref[...], mix, preferred_element_type=jnp.float32)
        result = jnp.where(live, xs[-d % PARTS][...].astype(jnp.float32) + projected, 0.0)
        out[:ROWS_W, :] = result.astype(jnp.bfloat16)
        pairs = result.reshape(WIN, 2, 8, PW)
        pairs = pairs[:, 0] + pairs[:, 1]
        terms = jnp.zeros((EXTRA, PW), jnp.float32)
        line = jnp.zeros((1, PW), jnp.float32)
        for i in range(MAX_LOCAL):
            held = jnp.sum(jnp.where(tiles[i], pairs, 0.0), axis=0)
            rest = jnp.sum(held, axis=0, keepdims=True) / lengths[i]
            line = line + rest
            for k in range(3):
                term = rest.astype(jnp.bfloat16).astype(jnp.float32)
                terms = jnp.where(term_ids == k * MAX_LOCAL + i, term, terms)
                rest = rest - term
        out[ROWS_W:, :] = terms.astype(jnp.bfloat16)
        sum_ref[0:1, :] = line[:, : PW // 2]
        sum_ref[1:2, :] = line[:, PW // 2 :]


def block(part, core, image, xs, weights):
    outs = jax.ShapeDtypeStruct((ROWS_W + EXTRA, PW), jnp.bfloat16)
    wide = pltpu.VMEM((ROWS_W, PW), jnp.bfloat16)
    return pl.pallas_call(
        block_kernel,
        grid_spec=pltpu.PrefetchScalarGridSpec(
            num_scalar_prefetch=3,
            grid=(1,),
            in_specs=[pl.BlockSpec(memory_space=pltpu.VMEM)] * len(xs)
            + [pl.BlockSpec(memory_space=pltpu.HBM)] * len(weights),
            out_specs=[pl.BlockSpec(memory_space=pltpu.VMEM)] * (2 * PARTS),
            scratch_shapes=[
                pltpu.VMEM((PARTS, ROWS_W, PW), jnp.bfloat16),
                wide,
                wide,
                wide,
                pltpu.VMEM((ROWS_W, D), jnp.bfloat16),
                pltpu.VMEM((PARTS, 4, D, PW), jnp.bfloat16),
                pltpu.SMEM((8,), jnp.int32),
                pltpu.SMEM((8,), jnp.int32),
                pltpu.SemaphoreType.DMA((5 * PARTS - 1,)),
            ],
        ),
        out_shape=[outs] * PARTS + [jax.ShapeDtypeStruct((2, PW // 2), jnp.float32)] * PARTS,
        compiler_params=MIDDLE,
        name="block",
    )(part, core, image, *xs, *weights)


def finish_kernel(part_ref, image_ref, r0, r1, r2, r3, out_ref, pooled_ref, out_vmem, sems):
    size = PART_SLOTS * TILE
    halo = ROWS_W - size
    received = (r0, r1, r2, r3)
    writes = []
    pooled = jnp.zeros((IMG, PW), jnp.float32)
    image_ids = lax.broadcasted_iota(jnp.int32, (IMG, PW), 0)
    for d, r in enumerate(received):
        p = (part_ref[0] + PARTS - d) % PARTS
        base = pl.multiple_of(p * size, size)
        before = received[(d + 1) % PARTS][size:ROWS_W, :]
        start = r[:halo, :] + jnp.where(p > 0, before, jnp.zeros_like(before))
        out_vmem[pl.ds(base, halo), :] = start
        out_vmem[pl.ds(pl.multiple_of(base + halo, TILE), size - halo), :] = r[halo:size, :]
        rows = pl.ds(base, size)
        writes.append(pltpu.make_async_copy(out_vmem.at[rows, :], out_ref.at[rows, :], sems.at[d]))
        writes[-1].start()
        first = jnp.where(p > 0, image_ref[jnp.maximum(p * PART_SLOTS - 1, 0)] + 1, 0)
        terms = r[ROWS_W:, :].astype(jnp.float32)
        for i in range(MAX_LOCAL):
            value = terms[i : i + 1] + terms[MAX_LOCAL + i : MAX_LOCAL + i + 1] + terms[2 * MAX_LOCAL + i : 2 * MAX_LOCAL + i + 1]
            pooled = pooled + jnp.where(image_ids == first + i, value, 0.0)
    pooled_ref[...] = pooled
    for write in writes:
        write.wait()


def finish(part, image, received):
    return pl.pallas_call(
        finish_kernel,
        grid_spec=pltpu.PrefetchScalarGridSpec(
            num_scalar_prefetch=2,
            grid=(1,),
            in_specs=[pl.BlockSpec(memory_space=pltpu.VMEM)] * PARTS,
            out_specs=[pl.BlockSpec(memory_space=pl.ANY), pl.BlockSpec((IMG, PW), lambda i, a, b: (0, 0))],
            scratch_shapes=[
                pltpu.VMEM((SLOTS * TILE, PW), jnp.bfloat16),
                pltpu.SemaphoreType.DMA((PARTS,)),
            ],
        ),
        out_shape=[
            jax.ShapeDtypeStruct((SLOTS * TILE, PW), jnp.bfloat16),
            jax.ShapeDtypeStruct((IMG, PW), jnp.float32),
        ],
        compiler_params=VMEM,
        name="finish",
    )(part, image, *received)


def pool_kernel(sums_ref, number_ref, pooled_ref, image_ref, out_ref):
    total = jnp.sum(sums_ref[...], axis=0)
    centre = jnp.concatenate([total[0:1], total[1:2]], axis=1) / number_ref[0:1, 0:1]
    slots = lax.broadcasted_iota(jnp.int32, (IMG, SLOTS), 0) == image_ref[...]
    present = jnp.max(jnp.where(slots, 1.0, 0.0), axis=1, keepdims=True) > 0.5
    out_ref[...] = jnp.where(present, pooled_ref[...] - centre, 0.0).astype(jnp.bfloat16)


def pool(sums, number, pooled, image):
    return pl.pallas_call(
        pool_kernel,
        in_specs=[pl.BlockSpec(memory_space=pltpu.VMEM)] * 4,
        out_shape=jax.ShapeDtypeStruct((IMG, PW), jnp.bfloat16),
        name="pool",
    )(sums, number, pooled, image)


def passed_on(pieces, shift):
    got = []
    for d in (1, 2, 3):
        got.append(lax.ppermute(pieces[d], "mp", shift(d)))
    return got


def whole_block(patches, dest_owner, dest_slot, packed_image, w_query, w_key, w_value, w_out):
    senders = lax.axis_size("dp")
    splits = lax.axis_size("mp")
    part = lax.axis_index("mp").astype(jnp.int32).reshape(1)
    core = (lax.axis_index("dp").astype(jnp.int32) & 1).reshape(1)
    near = lambda array: pltpu.with_memory_space_constraint(array, pltpu.VMEM)
    far = lambda array: pltpu.with_memory_space_constraint(array, pltpu.HBM)
    shift = lambda d: [(i, (i + d) % splits) for i in range(splits)]
    swap = [(i, i ^ 1) for i in range(senders)]

    own = (w_query, w_key, w_value, w_out)
    image = packed_image.reshape(1, SLOTS)
    outgoing, s0, s1 = send_pack(dest_owner, dest_slot, part, core, image, patches, own, senders)
    a0 = lax.ppermute(s0, "mp", shift(1))
    b1 = lax.ppermute(s1, "mp", shift(-1))
    a1 = lax.ppermute(s1, "mp", shift(1))
    b0 = lax.ppermute(s0, "mp", shift(-1))
    c0 = lax.ppermute(a0, "mp", shift(1))
    c1 = lax.ppermute(b1, "mp", shift(-1))
    a0x, a1x, b0x, b1x, c0x, c1x = (lax.ppermute(w, "dp", swap) for w in (a0, a1, b0, b1, c0, c1))
    weights = own + (a0, a1, a0x, a1x, b0, b1, b0x, b1x, c0, c1, c0x, c1x)

    incoming = lax.all_to_all(outgoing, "dp", split_axis=0, concat_axis=0, tiled=True)
    *windows, number = arrive_sort(part, near(incoming))
    rows = [windows[0]] + passed_on(windows, shift)
    outcome = block(part, core, packed_image, [near(r) for r in rows], [far(w) for w in weights])
    results, sums = outcome[:PARTS], outcome[PARTS:]
    total = sums[0] + sum(lax.ppermute(sums[d], "mp", shift(d)) for d in (1, 2, 3))
    received = [results[0]] + passed_on(results, shift)
    spread = jnp.broadcast_to(total[None], (senders, 2, PW // 2))
    gathered = lax.all_to_all(spread, "dp", split_axis=0, concat_axis=0, tiled=True)
    packed_out, pooled = finish(part, packed_image, [near(r) for r in received])
    pooled_out = pool(near(gathered), number, pooled, image)
    return (packed_out, pooled_out)


def solution(mesh):
    in_specs = (
        P("dp", None),
        P("dp"),
        P("dp"),
        P("dp"),
        P(None, "mp"),
        P(None, "mp"),
        P(None, "mp"),
        P("mp", None),
    )
    out_specs = (P("dp", "mp"), P("dp", "mp"))
    return jax.shard_map(whole_block, mesh=mesh, in_specs=in_specs, out_specs=out_specs, check_vma=False)
```
